128 devices in a mesh: dp: 2 (over z_lo), seq: 64 (over z_hi, y, x, core).
Axes of the slice: x: 4, y: 4, z: 4 (z_hi: 2, z_lo: 2; z = z_hi * 2 + z_lo), core: 2. Of those that a mesh axis runs over, the one named last changes fastest.
Arguments:
- grad_out: bfloat16 [2, 16384, 512], P('dp', 'seq'), may hold values from -6 to 6
- gate: bfloat16 [2, 16384, 512], P('dp', 'seq'), may hold values from -6 to 6
- signal: bfloat16 [2, 16384, 512], P('dp', 'seq'), may hold values from -6 to 6
- filters: float32 [2, 256, 16384], P(None, 'seq', 'dp'), may hold values from -0.046875 to 0.046875
Outputs:
- grad_signal: bfloat16 [2, 16384, 512], P('dp', 'seq')
- grad_gate: bfloat16 [2, 16384, 512], P('dp', 'seq')
- grad_filter: float32 [2, 256, 16384], P(None, 'seq', 'dp')
The draws below stay inside these ranges and needn't reach their ends.
All inputs are finite; a program needn't handle non-finite values.
Results may differ from the reference program's by a relative error of at most 0.005.
Values may be sent and summed in bfloat16 or wider, within the bound.
A program may use at most 128 MiB of HBM per device.

```python
import jax
import jax.numpy as jnp

SEG_CH = 256
SEGMENTS = 2
LEN = 16384
BATCH = 2


def block_levels(key, dims, split, smallest, high):
    def one(dim, shards_of):
        draws = jax.random.uniform(jax.random.fold_in(jax.random.fold_in(key, 6), dim), (shards_of,), jnp.float32, smallest / len(split), high / len(split))
        return jnp.repeat(jnp.exp(draws), dims[dim] // shards_of).reshape((-1,) + (1,) * (len(dims) - dim - 1))

    factor_of = one(*split[0])
    for cut in split[1:]:
        factor_of = factor_of * one(*cut)
    return factor_of


def noise(rng, extent, width, limit, shards=(), dtype=jnp.bfloat16):
    result = width * jax.random.normal(rng, extent, jnp.float32)
    if shards:
        result = result * block_levels(rng, extent, shards, -0.22, 0.18)
    return jnp.clip(result, -limit, limit).astype(dtype)


def setup_inputs(seed: int = 0) -> dict:
    arg_keys = jax.random.split(jax.random.key(seed), 5)
    grad_out = noise(arg_keys[0], (BATCH, LEN, SEGMENTS * SEG_CH), 1.0, 6.0, ((0, 2), (1, 64)))
    gate = noise(arg_keys[1], (BATCH, LEN, SEGMENTS * SEG_CH), 1.0, 6.0, ((0, 2), (1, 64)))
    signal = noise(arg_keys[2], (BATCH, LEN, SEGMENTS * SEG_CH), 1.0, 6.0, ((0, 2), (1, 64)))
    filters = noise(arg_keys[3], (SEGMENTS, SEG_CH, LEN), LEN ** -0.5, 0.046875, ((1, 64), (2, 2)), jnp.float32)
    return dict(grad_out=grad_out, gate=gate, signal=signal, filters=filters)


def forward_spectrum(values):
    return jnp.fft.rfft(values, n=2 * values.shape[-1], axis=-1)


def back_values(spectrum, length):
    return jnp.fft.irfft(spectrum, n=2 * length, axis=-1)[..., :length]


def reference(grad_out, gate, signal, filters):
    channels = SEGMENTS * SEG_CH
    gradient = grad_out.astype(jnp.float32)
    scaled = (gradient * gate.astype(jnp.float32)).astype(jnp.bfloat16)
    scaled_rows = jnp.transpose(scaled.astype(jnp.float32), (0, 2, 1))
    signal_rows = jnp.transpose(signal.astype(jnp.float32), (0, 2, 1))
    filter_spectrum = forward_spectrum(filters.reshape(channels, LEN))
    signal_spectrum = forward_spectrum(signal_rows)
    scaled_spectrum = forward_spectrum(scaled_rows)
    convolved = back_values(filter_spectrum * signal_spectrum, LEN).astype(jnp.bfloat16)
    adjoint = back_values(jnp.conj(filter_spectrum) * scaled_spectrum, LEN)
    kernels = back_values(scaled_spectrum * jnp.conj(signal_spectrum), LEN)
    grad_signal = jnp.transpose(adjoint, (0, 2, 1)).astype(jnp.bfloat16)
    conv_tokens = jnp.transpose(convolved, (0, 2, 1)).astype(jnp.float32)
    grad_gate = (gradient * conv_tokens).astype(jnp.bfloat16)
    factor = (BATCH * LEN) ** -0.5
    grad_filter = (jnp.sum(kernels, axis=0) * factor).reshape(SEGMENTS, SEG_CH, LEN)
    return grad_signal, grad_gate, grad_filter
```

```python
import functools
import math

import jax
import jax.numpy as jnp
import numpy as np
from jax import lax
from jax.experimental import pallas as pl
from jax.experimental.pallas import tpu as pltpu
from jax.sharding import PartitionSpec as P

MESH = pl.DeviceIdType.MESH
bf16 = jnp.bfloat16
f32 = jnp.float32

U = 256
HALF = U // 2


def split_table(table):
    high = jnp.asarray(table, f32).astype(bf16)
    low = (jnp.asarray(table, f32) - high.astype(f32)).astype(bf16)
    return high, low


def np_bf16(table):
    import ml_dtypes

    return np.asarray(table, np.float32).astype(ml_dtypes.bfloat16)


def np_split(table):
    high = np_bf16(table)
    low = np_bf16(np.asarray(table, np.float64) - high.astype(np.float64))
    return high, low


@functools.lru_cache(None)
def make_tables(rows):
    points = 2 * rows * U
    k1 = np.arange(rows)[:, None]
    i = np.arange(rows)[None, :]
    angle = 2 * np.pi * (i * (2 * k1 + 1) % (4 * rows)) / (4 * rows)
    outer = np.concatenate([np.cos(angle), -np.sin(angle)], 0)
    high, low = np_split(outer)
    forward = np.concatenate([high, low, high], 1)
    back_high, back_low = np_split(outer.T * (2.0 / points))
    back = np.concatenate([back_high, back_low, back_high], 1)
    u = np.arange(U)[None, :]
    turn = 2 * np.pi * (u * (2 * k1 + 1)) / (2 * points)
    twiddle = np.stack([np.cos(turn), -np.sin(turn)]).astype(np.float32)
    u0 = np.arange(HALF)[:, None]
    m = np.arange(HALF)[None, :]
    inner = []
    for p in range(2):
        a = 2 * np.pi * (u0 * (2 * m + p) % U) / U
        c, s = np.cos(a), np.sin(a)
        inner.append(np.block([[c, -s], [s, c]]))
    inner = np.stack(inner)
    inner_tables = np.stack(np_split(inner), 1)
    inverse_tables = np.stack(np_split(np.swapaxes(inner, 1, 2)), 1)
    return forward, back, twiddle, inner_tables, inverse_tables


@functools.lru_cache(None)
def make_permutation(pieces, segments, per_device):
    channels = pieces * segments * per_device
    table = np.zeros((channels, channels), np.float32)
    for j in range(pieces):
        for s in range(segments):
            for c in range(per_device):
                row = (j * segments + s) * per_device + c
                table[row, s * pieces * per_device + j * per_device + c] = 1
    return np_bf16(table)


def dot(a, b, dims=((1,), (0,))):
    return lax.dot_general(a, b, (dims, ((), ())), preferred_element_type=f32)


def split(x):
    high = x.astype(bf16)
    return high, (x - high.astype(f32)).astype(bf16)


def pack_kernel(grad_ref, gate_ref, signal_ref, filters_ref, perm_ref, pack_ref, pf_ref):
    pieces = pack_ref.shape[0]
    group = pf_ref.shape[1]
    per_device = filters_ref.shape[1]
    scaled = (grad_ref[...].astype(f32) * gate_ref[...].astype(f32)).astype(bf16)
    parts = []
    for x in (scaled, signal_ref[...]):
        rows = dot(perm_ref[...], x, ((1,), (1,)))
        parts.append(rows.reshape(pieces, group, x.shape[0]))
    pack_ref[...] = jnp.concatenate(parts, 1).astype(bf16)
    for s in range(filters_ref.shape[0]):
        for i in range(pf_ref.shape[0]):
            pf_ref[i, s * per_device : (s + 1) * per_device, :] = filters_ref[
                s, :, i * U : (i + 1) * U
            ]


def start_exchange(src_ref, dst_ref, send_sem, recv_sem):
    me = lax.axis_index("seq")
    pieces = src_ref.shape[0]

    def step(d, carry):
        peer = lax.rem(me + d, pieces)
        pltpu.make_async_remote_copy(
            src_ref=src_ref.at[peer],
            dst_ref=dst_ref.at[me],
            send_sem=send_sem,
            recv_sem=recv_sem,
            device_id={"seq": peer},
            device_id_type=MESH,
        ).start()
        return carry

    lax.fori_loop(1, pieces, step, 0)
    dst_ref[me] = src_ref[me]


def wait_exchange(src_ref, dst_ref, send_sem, recv_sem):
    pieces = src_ref.shape[0]
    whole = pltpu.make_async_remote_copy(
        src_ref=src_ref.at[pl.ds(0, pieces - 1)],
        dst_ref=dst_ref.at[pl.ds(0, pieces - 1)],
        send_sem=send_sem,
        recv_sem=recv_sem,
        device_id={"seq": lax.axis_index("seq")},
        device_id_type=MESH,
    )
    whole.wait_send()
    whole.wait_recv()


def meet(pieces):
    me = lax.axis_index("seq")
    other = 1 - lax.axis_index("dp")
    barrier = pltpu.get_barrier_semaphore()

    def greet(d, carry):
        pl.semaphore_signal(
            barrier, inc=1, device_id={"seq": lax.rem(me + d, pieces)}, device_id_type=MESH
        )
        return carry

    lax.fori_loop(1, pieces, greet, 0)
    pl.semaphore_signal(barrier, inc=1, device_id={"dp": other}, device_id_type=MESH)
    pl.semaphore_wait(barrier, pieces)


def scatter_kernel(pack_ref, pf_ref, recv_ref, filt_ref, send_sem, recv_sem, fsend, frecv):
    pieces = pack_ref.shape[0]
    half = pf_ref.shape[0]
    dp = lax.axis_index("dp")
    meet(pieces)
    mine = filt_ref.at[pl.ds(dp * half, half)]
    copy = pltpu.make_async_remote_copy(
        src_ref=pf_ref,
        dst_ref=mine,
        send_sem=fsend,
        recv_sem=frecv,
        device_id={"dp": 1 - dp},
        device_id_type=MESH,
    )
    copy.start()
    start_exchange(pack_ref, recv_ref, send_sem, recv_sem)
    mine[...] = pf_ref[...]
    copy.wait()
    wait_exchange(pack_ref, recv_ref, send_sem, recv_sem)


def gather_kernel(back_ref, ker_ref, rec_ref, ksum_ref, kbuf, send_sem, recv_sem, ksend, krecv):
    pieces = back_ref.shape[0]
    half = ksum_ref.shape[0]
    dp = lax.axis_index("dp")
    meet(pieces)
    copy = pltpu.make_async_remote_copy(
        src_ref=ker_ref.at[pl.ds((1 - dp) * half, half)],
        dst_ref=kbuf,
        send_sem=ksend,
        recv_sem=krecv,
        device_id={"dp": 1 - dp},
        device_id_type=MESH,
    )
    copy.start()
    start_exchange(back_ref, rec_ref, send_sem, recv_sem)
    copy.wait()
    ksum_ref[...] = ker_ref[pl.ds(dp * half, half)] + kbuf[...]
    wait_exchange(back_ref, rec_ref, send_sem, recv_sem)


def unpack_kernel(factor, rec_ref, ksum_ref, grad_ref, perm_ref, gs_ref, gg_ref, gf_ref):
    pieces, both, tokens = rec_ref.shape
    group = both // 2
    per_device = gf_ref.shape[1]
    rec = rec_ref[...].astype(f32)
    adjoint = rec[:, :group].reshape(pieces * group, tokens).astype(bf16)
    conv = rec[:, group:].reshape(pieces * group, tokens).astype(bf16)
    gs_ref[...] = dot(adjoint, perm_ref[...], ((0,), (0,))).astype(bf16)
    conv_tokens = dot(conv, perm_ref[...], ((0,), (0,)))
    gg_ref[...] = (grad_ref[...].astype(f32) * conv_tokens).astype(bf16)
    for s in range(gf_ref.shape[0]):
        for i in range(ksum_ref.shape[0]):
            gf_ref[s, :, i * U : (i + 1) * U] = (
                ksum_ref[i, s * per_device : (s + 1) * per_device, :] * factor
            )


def spectral_kernel(
    recv_ref, filt_ref, fwd_ref, back_ref, tw_ref, in_ref, inv_ref, out_ref, ker_ref, xs, fs, ys, ks
):
    rows, both, _ = recv_ref.shape
    group = both // 2
    for h in range(2):
        lanes = slice(h * HALF, (h + 1) * HALF)
        xs[h] = recv_ref[:, :, lanes].astype(f32).reshape(rows * both, HALF)
        fs[h] = filt_ref[:, lanes]

    def take(ref, c, count):
        return jnp.concatenate([ref[h, pl.ds(c, rows, stride=count), :] for h in range(2)], 1)

    def put(ref, c, count, value):
        for h in range(2):
            ref[h, pl.ds(c, rows, stride=count), :] = value[:, h * HALF : (h + 1) * HALF]

    def forward(p):
        pr, pi = p[:rows], p[rows:]
        tr, ti = tw_ref[0], tw_ref[1]
        qr = pr * tr - pi * ti
        qi = pr * ti + pi * tr
        a = jnp.concatenate([qr[:, :HALF], qi[:, :HALF]], 1)
        b = jnp.concatenate([qr[:, HALF:], qi[:, HALF:]], 1)
        return a + b, a - b

    def three(x, table_ref, p):
        high, low = split(x)
        return (
            dot(high, table_ref[p, 0]) + dot(low, table_ref[p, 0]) + dot(high, table_ref[p, 1])
        )

    def body(c, carry):
        g = take(xs, c, both).astype(bf16)
        s = take(xs, c + group, both).astype(bf16)
        fh, fl = split(take(fs, c, group))
        short = fwd_ref[:, : 2 * rows]
        stages = [
            dot(fwd_ref[...], jnp.concatenate([fh, fh, fl], 0)),
            dot(short, jnp.concatenate([g, g], 0)),
            dot(short, jnp.concatenate([s, s], 0)),
        ]
        turned = [forward(p) for p in stages]
        parts = []
        for p in range(2):
            spec = three(jnp.concatenate([t[p] for t in turned], 0), in_ref, p)
            fr, fi = spec[:rows, :HALF], spec[:rows, HALF:]
            gr, gi = spec[rows : 2 * rows, :HALF], spec[rows : 2 * rows, HALF:]
            sr, si = spec[2 * rows :, :HALF], spec[2 * rows :, HALF:]
            adj = jnp.concatenate([fr * gr + fi * gi, fr * gi - fi * gr], 1)
            conv = jnp.concatenate([fr * sr - fi * si, fr * si + fi * sr], 1)
            ker = jnp.concatenate([gr * sr + gi * si, gi * sr - gr * si], 1)
            parts.append(three(jnp.concatenate([adj, conv, ker], 0), inv_ref, p))
        plus, minus = parts[0] + parts[1], parts[0] - parts[1]
        tr, ti = tw_ref[0], tw_ref[1]
        results = []
        for n in range(3):
            here = slice(n * rows, (n + 1) * rows)
            zr = jnp.concatenate([plus[here, :HALF], minus[here, :HALF]], 1)
            zi = jnp.concatenate([plus[here, HALF:], minus[here, HALF:]], 1)
            z = jnp.concatenate([zr * tr + zi * ti, zi * tr - zr * ti], 0)
            high, low = split(z)
            results.append(dot(back_ref[...], jnp.concatenate([high, high, low], 0)))
        put(ys, c, both, results[0])
        put(ys, c + group, both, results[1])
        put(ks, c, group, results[2])
        return carry

    lax.fori_loop(0, group, body, 0, unroll=UNROLL)
    for h in range(2):
        lanes = slice(h * HALF, (h + 1) * HALF)
        out_ref[:, :, lanes] = ys[h].reshape(rows, both, HALF).astype(bf16)
        ker_ref[:, lanes] = ks[h]


UNROLL = 2


def vmem(count):
    return [pl.BlockSpec(memory_space=pltpu.VMEM)] * count


def spectral(recv, filt, tables):
    rows, both, _ = recv.shape
    group = both // 2
    out, ker = pl.pallas_call(
        spectral_kernel,
        out_shape=(
            jax.ShapeDtypeStruct(recv.shape, bf16),
            jax.ShapeDtypeStruct((rows * group, U), f32),
        ),
        in_specs=vmem(7),
        out_specs=tuple(vmem(2)),
        scratch_shapes=[
            pltpu.VMEM((2, rows * both, HALF), f32),
            pltpu.VMEM((2, rows * group, HALF), f32),
            pltpu.VMEM((2, rows * both, HALF), f32),
            pltpu.VMEM((2, rows * group, HALF), f32),
        ],
        name="spectral",
    )(recv, filt.reshape(rows * group, U), *tables)
    return out, ker.reshape(rows, group, U)


def on_device(grad_out, gate, signal, filters):
    tokens, channels = grad_out.shape[1:]
    pieces = lax.axis_size("seq")
    halves = lax.axis_size("dp")
    segments, per_device, part = filters.shape
    group = segments * per_device
    rows = part * halves // U
    half = part // U
    tables = [jnp.asarray(t) for t in make_tables(rows)]
    perm = jnp.asarray(make_permutation(pieces, segments, per_device))
    gradient = grad_out[0]
    pack, pf = pl.pallas_call(
        pack_kernel,
        out_shape=(
            jax.ShapeDtypeStruct((pieces, 2 * group, tokens), bf16),
            jax.ShapeDtypeStruct((half, group, U), f32),
        ),
        in_specs=vmem(5),
        out_specs=tuple(vmem(2)),
        name="pack",
    )(gradient, gate[0], signal[0], filters, perm)
    dma = pltpu.SemaphoreType.DMA
    recv, filt = pl.pallas_call(
        scatter_kernel,
        out_shape=(
            jax.ShapeDtypeStruct((pieces, 2 * group, tokens), bf16),
            jax.ShapeDtypeStruct((rows, group, U), f32),
        ),
        in_specs=vmem(2),
        out_specs=tuple(vmem(2)),
        scratch_shapes=[dma, dma, dma, dma],
        compiler_params=pltpu.CompilerParams(collective_id=0, has_side_effects=True),
        name="scatter",
    )(pack, pf)
    back, ker = spectral(recv, filt, tables)
    rec, ksum = pl.pallas_call(
        gather_kernel,
        out_shape=(
            jax.ShapeDtypeStruct((pieces, 2 * group, tokens), bf16),
            jax.ShapeDtypeStruct((half, group, U), f32),
        ),
        in_specs=vmem(2),
        out_specs=tuple(vmem(2)),
        scratch_shapes=[pltpu.VMEM((half, group, U), f32), dma, dma, dma, dma],
        compiler_params=pltpu.CompilerParams(collective_id=1, has_side_effects=True),
        name="gather",
    )(back, ker)
    factor = (halves * rows * U) ** (-0.5)
    grad_signal, grad_gate, grad_filter = pl.pallas_call(
        functools.partial(unpack_kernel, factor),
        out_shape=(
            jax.ShapeDtypeStruct((tokens, channels), bf16),
            jax.ShapeDtypeStruct((tokens, channels), bf16),
            jax.ShapeDtypeStruct((segments, per_device, part), f32),
        ),
        in_specs=vmem(4),
        out_specs=tuple(vmem(3)),
        name="unpack",
    )(rec, ksum, gradient, perm)
    return grad_signal[None], grad_gate[None], grad_filter


def solution(mesh):
    placed = (
        P("dp", "seq", None),
        P("dp", "seq", None),
        P("dp", "seq", None),
        P(None, "seq", "dp"),
    )
    return jax.shard_map(
        on_device,
        mesh=mesh,
        in_specs=placed,
        out_specs=(P("dp", "seq", None), P("dp", "seq", None), P(None, "seq", "dp")),
        check_vma=False,
    )
```

```python
import functools
import math

import jax
import jax.numpy as jnp
import numpy as np
from jax import lax
from jax.experimental import pallas as pl
from jax.experimental.pallas import tpu as pltpu
from jax.sharding import PartitionSpec as P

MESH = pl.DeviceIdType.MESH
bf16 = jnp.bfloat16
f32 = jnp.float32

U = 256
HALF = U // 2


def split_table(table):
    high = jnp.asarray(table, f32).astype(bf16)
    low = (jnp.asarray(table, f32) - high.astype(f32)).astype(bf16)
    return high, low


def np_bf16(table):
    import ml_dtypes

    return np.asarray(table, np.float32).astype(ml_dtypes.bfloat16)


def np_split(table):
    high = np_bf16(table)
    low = np_bf16(np.asarray(table, np.float64) - high.astype(np.float64))
    return high, low


@functools.lru_cache(None)
def make_tables(rows):
    points = 2 * rows * U
    k1 = np.arange(rows)[:, None]
    i = np.arange(rows)[None, :]
    angle = 2 * np.pi * (i * (2 * k1 + 1) % (4 * rows)) / (4 * rows)
    outer = np.concatenate([np.cos(angle), -np.sin(angle)], 0)
    high, low = np_split(outer)
    forward = np.concatenate([high, low, high], 1)
    back_high, back_low = np_split(outer.T * (2.0 / points))
    back = np.concatenate([back_high, back_low, back_high], 1)
    u = np.arange(U)[None, :]
    turn = 2 * np.pi * (u * (2 * k1 + 1)) / (2 * points)
    twiddle = np.stack([np.cos(turn), -np.sin(turn)]).astype(np.float32)
    u0 = np.arange(HALF)[:, None]
    m = np.arange(HALF)[None, :]
    inner = []
    for p in range(2):
        a = 2 * np.pi * (u0 * (2 * m + p) % U) / U
        c, s = np.cos(a), np.sin(a)
        inner.append(np.block([[c, -s], [s, c]]))
    inner = np.stack(inner)
    inner_tables = np.stack(np_split(inner), 1)
    inverse_tables = np.stack(np_split(np.swapaxes(inner, 1, 2)), 1)
    return forward, back, twiddle, inner_tables, inverse_tables


@functools.lru_cache(None)
def make_permutation(pieces, per_device):
    width = pieces * per_device
    row = np.arange(2 * width)
    j, rest = np.divmod(row, 2 * per_device)
    tensor, c = np.divmod(rest, per_device)
    table = np.zeros((2 * width, 2 * width), np.float32)
    table[row, tensor * width + j * per_device + c] = 1
    return np_bf16(table)


def dot(a, b, dims=((1,), (0,))):
    return lax.dot_general(a, b, (dims, ((), ())), preferred_element_type=f32)


def split(x):
    high = x.astype(bf16)
    return high, (x - high.astype(f32)).astype(bf16)


def peer_copy(src_ref, dst_ref, send_sem, recv_sem, peer):
    return pltpu.make_async_remote_copy(
        src_ref=src_ref,
        dst_ref=dst_ref,
        send_sem=send_sem,
        recv_sem=recv_sem,
        device_id=peer,
        device_id_type=MESH,
    )


def start_exchange(src_ref, dst_ref, send_sem, recv_sem):
    me = lax.axis_index("seq")
    pieces = src_ref.shape[0]

    def step(d, carry):
        peer = lax.rem(me + d, pieces)
        peer_copy(
            src_ref.at[peer], dst_ref.at[me], send_sem, recv_sem, {"seq": peer}
        ).start()
        return carry

    lax.fori_loop(1, pieces, step, 0)
    dst_ref[me] = src_ref[me]


def all_of(src_ref, dst_ref, send_sem, recv_sem):
    others = pl.ds(0, src_ref.shape[0] - 1)
    return peer_copy(
        src_ref.at[others],
        dst_ref.at[others],
        send_sem,
        recv_sem,
        {"seq": lax.axis_index("seq")},
    )


def greet_all(pieces):
    me = lax.axis_index("seq")
    barrier = pltpu.get_barrier_semaphore()

    def greet(d, carry):
        pl.semaphore_signal(
            barrier, inc=1, device_id={"seq": lax.rem(me + d, pieces)}, device_id_type=MESH
        )
        return carry

    lax.fori_loop(1, pieces, greet, 0)
    pl.semaphore_signal(
        barrier, inc=1, device_id={"dp": 1 - lax.axis_index("dp")}, device_id_type=MESH
    )
    return barrier


def take(ref, c, rows, stride):
    return jnp.concatenate([ref[h, pl.ds(c, rows, stride=stride), :] for h in range(2)], 1)


def put(ref, c, rows, stride, value):
    for h in range(2):
        ref[h, pl.ds(c, rows, stride=stride), :] = value[:, h * HALF : (h + 1) * HALF]


def turn(p, tw_ref):
    rows = p.shape[0] // 2
    pr, pi = p[:rows], p[rows:]
    tr, ti = tw_ref[0], tw_ref[1]
    qr = pr * tr - pi * ti
    qi = pr * ti + pi * tr
    a = jnp.concatenate([qr[:, :HALF], qi[:, :HALF]], 1)
    b = jnp.concatenate([qr[:, HALF:], qi[:, HALF:]], 1)
    return a + b, a - b


def unturn(plus, minus, tw_ref):
    tr, ti = tw_ref[0], tw_ref[1]
    zr = jnp.concatenate([plus[:, :HALF], minus[:, :HALF]], 1)
    zi = jnp.concatenate([plus[:, HALF:], minus[:, HALF:]], 1)
    return jnp.concatenate([zr * tr + zi * ti, zi * tr - zr * ti], 0)


def three(x, table_ref, p):
    high, low = split(x)
    return dot(high, table_ref[p, 0]) + dot(low, table_ref[p, 0]) + dot(high, table_ref[p, 1])


def main_kernel(
    grad_ref,
    gate_ref,
    signal_ref,
    filters_ref,
    perm_ref,
    fwd_ref,
    inner_back_ref,
    tw_ref,
    in_ref,
    inv_ref,
    rec_ref,
    ksum_ref,
    pack,
    recv,
    back,
    pf,
    filt,
    fs,
    fspec,
    xs,
    ys,
    ks,
    ker,
    kbuf,
    send_in,
    recv_in,
    send_out,
    recv_out,
    fsend,
    frecv,
    ksend,
    krecv,
):
    segments, pieces, group, tokens = pack.shape
    per_device = group // 2
    rows = pieces * tokens // U
    part = pf.shape[1]
    dp = lax.axis_index("dp")
    partner = {"dp": 1 - dp}
    barrier = greet_all(pieces)

    for s in range(segments):
        for i in range(part // per_device):
            pf[s, i * per_device : (i + 1) * per_device, :] = filters_ref[
                s, :, i * U : (i + 1) * U
            ]
    width = pieces * per_device
    for s in range(segments):
        here = slice(s * width, (s + 1) * width)
        scaled = (grad_ref[:, here].astype(f32) * gate_ref[:, here].astype(f32)).astype(bf16)
        joined = jnp.concatenate([scaled, signal_ref[:, here]], 1)
        moved = dot(perm_ref[...], joined, ((1,), (1,)))
        pack[s] = moved.reshape(pieces, group, tokens).astype(bf16)

    pl.semaphore_wait(barrier, pieces)
    mine = filt.at[:, pl.ds(dp * part, part)]
    filter_copy = peer_copy(pf, mine, fsend, frecv, partner)
    filter_copy.start()
    for s in range(segments):
        start_exchange(pack.at[s], recv.at[s], send_in.at[s], recv_in.at[s])
    mine[...] = pf[...]
    filter_copy.wait()

    for h in range(2):
        lanes = slice(h * HALF, (h + 1) * HALF)
        for s in range(segments):
            fs[s, h] = filt[s, :, lanes]

    for s in range(segments):

        def filter_step(n, carry, s=s):
            stages = []
            for c in (2 * n, 2 * n + 1):
                high, low = split(take(fs.at[s], c, rows, per_device))
                stages.append(
                    turn(dot(fwd_ref[...], jnp.concatenate([high, high, low], 0)), tw_ref)
                )
            at = pl.multiple_of(n * 2 * rows, 2 * rows)
            for p in range(2):
                fspec[s, p, pl.ds(at, 2 * rows)] = three(
                    jnp.concatenate([t[p] for t in stages], 0), in_ref, p
                )
            return carry

        lax.fori_loop(0, per_device // 2, filter_step, 0)

    short = fwd_ref[:, : 2 * rows]
    for s in range(segments):
        incoming = all_of(pack.at[s], recv.at[s], send_in.at[s], recv_in.at[s])
        incoming.wait_recv()
        for h in range(2):
            lanes = slice(h * HALF, (h + 1) * HALF)
            xs[h] = recv[s, :, :, lanes].astype(f32).reshape(rows * group, HALF)

        def step(c, carry, s=s):
            turned = []
            for r in (c, c + per_device):
                x = take(xs, r, rows, group).astype(bf16)
                turned.append(turn(dot(short, jnp.concatenate([x, x], 0)), tw_ref))
            at = pl.multiple_of(c * rows, rows)
            parts = []
            for p in range(2):
                spec = three(jnp.concatenate([t[p] for t in turned], 0), in_ref, p)
                fr = fspec[s, p, pl.ds(at, rows), :HALF]
                fi = fspec[s, p, pl.ds(at, rows), HALF:]
                gr, gi = spec[:rows, :HALF], spec[:rows, HALF:]
                sr, si = spec[rows:, :HALF], spec[rows:, HALF:]
                adj = jnp.concatenate([fr * gr + fi * gi, fr * gi - fi * gr], 1)
                conv = jnp.concatenate([fr * sr - fi * si, fr * si + fi * sr], 1)
                kernels = jnp.concatenate([gr * sr + gi * si, gi * sr - gr * si], 1)
                parts.append(three(jnp.concatenate([adj, conv, kernels], 0), inv_ref, p))
            plus, minus = parts[0] + parts[1], parts[0] - parts[1]
            results = []
            for n in range(3):
                here = slice(n * rows, (n + 1) * rows)
                high, low = split(unturn(plus[here], minus[here], tw_ref))
                results.append(
                    dot(inner_back_ref[...], jnp.concatenate([high, high, low], 0))
                )
            put(ys, c, rows, group, results[0])
            put(ys, c + per_device, rows, group, results[1])
            put(ks, c, rows, per_device, results[2])
            return carry

        lax.fori_loop(0, per_device, step, 0, unroll=UNROLL)
        for h in range(2):
            lanes = slice(h * HALF, (h + 1) * HALF)
            back[s, :, :, lanes] = ys[h].reshape(pieces, group, HALF).astype(bf16)
            ker[s, :, lanes] = ks[h]
        start_exchange(back.at[s], rec_ref.at[s], send_out.at[s], recv_out.at[s])
        peer_copy(
            ker.at[s, pl.ds((1 - dp) * part, part)], kbuf.at[s], ksend.at[s], krecv.at[s], partner
        ).start()

    for s in range(segments):
        peer_copy(
            ker.at[s, pl.ds((1 - dp) * part, part)], kbuf.at[s], ksend.at[s], krecv.at[s], partner
        ).wait()
        ksum_ref[s] = ker[s, pl.ds(dp * part, part)] + kbuf[s]
    for s in range(segments):
        all_of(pack.at[s], recv.at[s], send_in.at[s], recv_in.at[s]).wait_send()
        outgoing = all_of(back.at[s], rec_ref.at[s], send_out.at[s], recv_out.at[s])
        outgoing.wait_send()
        outgoing.wait_recv()


UNROLL = 2


def unpack_kernel(factor, rec_ref, ksum_ref, grad_ref, perm_ref, gs_ref, gg_ref, gf_ref):
    segments, pieces, group, tokens = rec_ref.shape
    per_device = group // 2
    width = pieces * per_device
    for s in range(segments):
        here = slice(s * width, (s + 1) * width)
        rec = rec_ref[s].astype(f32).reshape(pieces * group, tokens).astype(bf16)
        both = dot(rec, perm_ref[...], ((0,), (0,)))
        gs_ref[:, here] = both[:, :width].astype(bf16)
        gg_ref[:, here] = (grad_ref[:, here].astype(f32) * both[:, width:]).astype(bf16)
        for i in range(ksum_ref.shape[1] // per_device):
            gf_ref[s, :, i * U : (i + 1) * U] = (
                ksum_ref[s, i * per_device : (i + 1) * per_device, :] * factor
            )


def vmem(count):
    return [pl.BlockSpec(memory_space=pltpu.VMEM)] * count


def on_device(grad_out, gate, signal, filters):
    tokens, channels = grad_out.shape[1:]
    pieces = lax.axis_size("seq")
    halves = lax.axis_size("dp")
    segments, per_device, length = filters.shape
    group = 2 * per_device
    rows = length * halves // U
    part = length // U * per_device
    tables = [jnp.asarray(t) for t in make_tables(rows)]
    perm = jnp.asarray(make_permutation(pieces, per_device))
    gradient = grad_out[0]
    dma = pltpu.SemaphoreType.DMA
    blocks = (segments, pieces, group, tokens)
    rec, ksum = pl.pallas_call(
        main_kernel,
        out_shape=(
            jax.ShapeDtypeStruct(blocks, bf16),
            jax.ShapeDtypeStruct((segments, part, U), f32),
        ),
        in_specs=vmem(10),
        out_specs=tuple(vmem(2)),
        scratch_shapes=[
            pltpu.VMEM(blocks, bf16),
            pltpu.VMEM(blocks, bf16),
            pltpu.VMEM(blocks, bf16),
            pltpu.VMEM((segments, part, U), f32),
            pltpu.VMEM((segments, part * halves, U), f32),
            pltpu.VMEM((segments, 2, rows * per_device, HALF), f32),
            pltpu.VMEM((segments, 2, rows * per_device, U), f32),
            pltpu.VMEM((2, rows * group, HALF), f32),
            pltpu.VMEM((2, rows * group, HALF), f32),
            pltpu.VMEM((2, rows * per_device, HALF), f32),
            pltpu.VMEM((segments, part * halves, U), f32),
            pltpu.VMEM((segments, part, U), f32),
            dma((segments,)),
            dma((segments,)),
            dma((segments,)),
            dma((segments,)),
            dma,
            dma,
            dma((segments,)),
            dma((segments,)),
        ],
        compiler_params=pltpu.CompilerParams(collective_id=0, has_side_effects=True),
        name="main",
    )(gradient, gate[0], signal[0], filters, perm, *tables)
    factor = (halves * rows * U) ** (-0.5)
    grad_signal, grad_gate, grad_filter = pl.pallas_call(
        functools.partial(unpack_kernel, factor),
        out_shape=(
            jax.ShapeDtypeStruct((tokens, channels), bf16),
            jax.ShapeDtypeStruct((tokens, channels), bf16),
            jax.ShapeDtypeStruct(filters.shape, f32),
        ),
        in_specs=vmem(4),
        out_specs=tuple(vmem(3)),
        name="unpack",
    )(rec, ksum, gradient, perm)
    return grad_signal[None], grad_gate[None], grad_filter


def solution(mesh):
    placed = (
        P("dp", "seq", None),
        P("dp", "seq", None),
        P("dp", "seq", None),
        P(None, "seq", "dp"),
    )
    return jax.shard_map(
        on_device,
        mesh=mesh,
        in_specs=placed,
        out_specs=(P("dp", "seq", None), P("dp", "seq", None), P(None, "seq", "dp")),
        check_vma=False,
    )
```

```python
import functools
import math

import jax
import jax.numpy as jnp
import numpy as np
from jax import lax
from jax.experimental import pallas as pl
from jax.experimental.pallas import tpu as pltpu
from jax.sharding import PartitionSpec as P

MESH = pl.DeviceIdType.MESH
bf16 = jnp.bfloat16
f32 = jnp.float32

U = 256
HALF = U // 2


def split_table(table):
    high = jnp.asarray(table, f32).astype(bf16)
    low = (jnp.asarray(table, f32) - high.astype(f32)).astype(bf16)
    return high, low


def np_bf16(table):
    import ml_dtypes

    return np.asarray(table, np.float32).astype(ml_dtypes.bfloat16)


def np_split(table):
    high = np_bf16(table)
    low = np_bf16(np.asarray(table, np.float64) - high.astype(np.float64))
    return high, low


@functools.lru_cache(None)
def make_tables(rows):
    points = 2 * rows * U
    k1 = np.arange(rows)[:, None]
    i = np.arange(rows)[None, :]
    angle = 2 * np.pi * (i * (2 * k1 + 1) % (4 * rows)) / (4 * rows)
    outer = np.concatenate([np.cos(angle), -np.sin(angle)], 0)
    high, low = np_split(outer)
    forward = np.concatenate([high, low, high], 1)
    back_high, back_low = np_split(outer.T * (2.0 / points))
    back = np.concatenate([back_high, back_low, back_high], 1)
    u = np.arange(U)[None, :]
    turn = 2 * np.pi * (u * (2 * k1 + 1)) / (2 * points)
    twiddle = np.stack([np.cos(turn), -np.sin(turn)]).astype(np.float32)
    u0 = np.arange(HALF)[:, None]
    m = np.arange(HALF)[None, :]
    inner = []
    for p in range(2):
        a = 2 * np.pi * (u0 * (2 * m + p) % U) / U
        c, s = np.cos(a), np.sin(a)
        inner.append(np.block([[c, -s], [s, c]]))
    inner = np.stack(inner)
    inner_tables = np.stack(np_split(inner), 1)
    inverse_tables = np.stack(np_split(np.swapaxes(inner, 1, 2)), 1)
    return forward, back, twiddle, inner_tables, inverse_tables


@functools.lru_cache(None)
def make_permutation(pieces, per_device):
    width = pieces * per_device
    row = np.arange(2 * width)
    j, rest = np.divmod(row, 2 * per_device)
    tensor, c = np.divmod(rest, per_device)
    table = np.zeros((2 * width, 2 * width), np.float32)
    table[row, tensor * width + j * per_device + c] = 1
    return np_bf16(table)


def dot(a, b, dims=((1,), (0,))):
    return lax.dot_general(a, b, (dims, ((), ())), preferred_element_type=f32)


def split(x):
    high = x.astype(bf16)
    return high, (x - high.astype(f32)).astype(bf16)


def peer_copy(src_ref, dst_ref, send_sem, recv_sem, peer):
    return pltpu.make_async_remote_copy(
        src_ref=src_ref,
        dst_ref=dst_ref,
        send_sem=send_sem,
        recv_sem=recv_sem,
        device_id=peer,
        device_id_type=MESH,
    )


def nth_peer(me, n, pieces):
    def far(v):
        return v + (v // 2) * (5 - 2 * v)

    core = lax.rem(lax.rem(me, 2) + lax.rem(n, 2), 2)
    x = lax.rem(lax.rem(me // 2, 4) + far(lax.rem(n // 2, 4)), 4)
    y = lax.rem(lax.rem(me // 8, 4) + far(lax.rem(n // 8, 4)), 4)
    z = lax.rem(me // 32 + n // 32, 2)
    return ((z * 4 + y) * 4 + x) * 2 + core


def start_exchange(src_ref, dst_ref, send_sem, recv_sem):
    me = lax.axis_index("seq")
    pieces = src_ref.shape[0]

    def step(n, carry):
        peer = nth_peer(me, pieces - n, pieces)
        peer_copy(
            src_ref.at[peer], dst_ref.at[me], send_sem, recv_sem, {"seq": peer}
        ).start()
        return carry

    lax.fori_loop(1, pieces, step, 0)
    dst_ref[me] = src_ref[me]


def all_of(src_ref, dst_ref, send_sem, recv_sem):
    others = pl.ds(0, src_ref.shape[0] - 1)
    return peer_copy(
        src_ref.at[others],
        dst_ref.at[others],
        send_sem,
        recv_sem,
        {"seq": lax.axis_index("seq")},
    )


def greet_all(pieces):
    me = lax.axis_index("seq")
    barrier = pltpu.get_barrier_semaphore()

    def greet(d, carry):
        pl.semaphore_signal(
            barrier, inc=1, device_id={"seq": lax.rem(me + d, pieces)}, device_id_type=MESH
        )
        return carry

    lax.fori_loop(1, pieces, greet, 0)
    pl.semaphore_signal(
        barrier, inc=1, device_id={"dp": 1 - lax.axis_index("dp")}, device_id_type=MESH
    )
    return barrier


def take(ref, c, rows, stride):
    return jnp.concatenate([ref[h, pl.ds(c, rows, stride=stride), :] for h in range(2)], 1)


def put(ref, c, rows, stride, value):
    for h in range(2):
        ref[h, pl.ds(c, rows, stride=stride), :] = value[:, h * HALF : (h + 1) * HALF]


def turn(p, tw_ref):
    rows = p.shape[0] // 2
    pr, pi = p[:rows], p[rows:]
    tr, ti = tw_ref[0], tw_ref[1]
    qr = pr * tr - pi * ti
    qi = pr * ti + pi * tr
    a = jnp.concatenate([qr[:, :HALF], qi[:, :HALF]], 1)
    b = jnp.concatenate([qr[:, HALF:], qi[:, HALF:]], 1)
    return a + b, a - b


def unturn(plus, minus, tw_ref):
    tr, ti = tw_ref[0], tw_ref[1]
    zr = jnp.concatenate([plus[:, :HALF], minus[:, :HALF]], 1)
    zi = jnp.concatenate([plus[:, HALF:], minus[:, HALF:]], 1)
    return jnp.concatenate([zr * tr + zi * ti, zi * tr - zr * ti], 0)


def three(x, table_ref, p):
    high, low = split(x)
    return dot(high, table_ref[p, 0]) + dot(low, table_ref[p, 0]) + dot(high, table_ref[p, 1])


def main_kernel(*refs):
    operands, refs = refs[:10], refs[10:]
    rec_ref, ksum_ref = refs[:2]
    held, refs = refs[2:12], refs[12:]
    grad_ref, gate_ref, signal_ref, filters_ref, perm_ref = held[:5]
    fwd_ref, inner_back_ref, tw_ref, in_ref, inv_ref = held[5:]
    pack, recv, back, pf, pfin, fs, fspec, xs, ys, ks, kout, kbuf = refs[:12]
    send_in, recv_in, send_out, recv_out, fsend, frecv, ksend, krecv, load_sem = refs[12:]
    segments, pieces, group, tokens = pack.shape
    per_device = group // 2
    rows = pieces * tokens // U
    part = pf.shape[1]
    dp = lax.axis_index("dp")
    partner = {"dp": 1 - dp}
    loads = [
        pltpu.make_async_copy(operands[n], held[n], load_sem.at[n]) for n in range(len(held))
    ]
    for n in (3, 0, 1, 2, 4, 5, 6, 7, 8, 9):
        loads[n].start()
    barrier = greet_all(pieces)

    loads[3].wait()
    own = dp * part
    other = (1 - dp) * part
    for s in range(segments):
        for i in range(part // per_device):
            for h in range(2):
                fs[s, h, pl.ds(own + i * per_device, per_device), :] = filters_ref[
                    s, :, i * U + h * HALF : i * U + (h + 1) * HALF
                ]
        for h in range(2):
            pf[s, :, h * HALF : (h + 1) * HALF] = fs[s, h, pl.ds(own, part)].astype(bf16)
    for n in (0, 1, 2, 4):
        loads[n].wait()
    width = pieces * per_device
    for s in range(segments):
        here = slice(s * width, (s + 1) * width)
        scaled = (grad_ref[:, here].astype(f32) * gate_ref[:, here].astype(f32)).astype(bf16)
        joined = jnp.concatenate([scaled, signal_ref[:, here]], 1)
        moved = dot(perm_ref[...], joined, ((1,), (1,)))
        pack[s] = moved.reshape(pieces, group, tokens).astype(bf16)

    pl.semaphore_wait(barrier, pieces)
    filter_copy = peer_copy(pf, pfin, fsend, frecv, partner)
    filter_copy.start()
    for s in range(segments):
        start_exchange(pack.at[s], recv.at[s], send_in.at[s], recv_in.at[s])
    for n in range(5, 10):
        loads[n].wait()
    filter_copy.wait()
    for h in range(2):
        lanes = slice(h * HALF, (h + 1) * HALF)
        for s in range(segments):
            fs[s, h, pl.ds(other, part)] = pfin[s, :, lanes].astype(f32)

    for s in range(segments):

        def filter_step(n, carry, s=s):
            stages = []
            for c in (2 * n, 2 * n + 1):
                high, low = split(take(fs.at[s], c, rows, per_device))
                stages.append(
                    turn(dot(fwd_ref[...], jnp.concatenate([high, high, low], 0)), tw_ref)
                )
            at = pl.multiple_of(n * 2 * rows, 2 * rows)
            for p in range(2):
                fspec[s, p, pl.ds(at, 2 * rows)] = three(
                    jnp.concatenate([t[p] for t in stages], 0), in_ref, p
                )
            return carry

        lax.fori_loop(0, per_device // 2, filter_step, 0)

    short = fwd_ref[:, : 2 * rows]
    for s in range(segments):
        incoming = all_of(pack.at[s], recv.at[s], send_in.at[s], recv_in.at[s])
        incoming.wait_recv()
        for h in range(2):
            lanes = slice(h * HALF, (h + 1) * HALF)
            xs[h] = recv[s, :, :, lanes].astype(f32).reshape(rows * group, HALF)

        def step(c, carry, s=s):
            turned = []
            for r in (c, c + per_device):
                x = take(xs, r, rows, group).astype(bf16)
                turned.append(turn(dot(short, jnp.concatenate([x, x], 0)), tw_ref))
            at = pl.multiple_of(c * rows, rows)
            parts = []
            for p in range(2):
                spec = three(jnp.concatenate([t[p] for t in turned], 0), in_ref, p)
                fr = fspec[s, p, pl.ds(at, rows), :HALF]
                fi = fspec[s, p, pl.ds(at, rows), HALF:]
                gr, gi = spec[:rows, :HALF], spec[:rows, HALF:]
                sr, si = spec[rows:, :HALF], spec[rows:, HALF:]
                adj = jnp.concatenate([fr * gr + fi * gi, fr * gi - fi * gr], 1)
                conv = jnp.concatenate([fr * sr - fi * si, fr * si + fi * sr], 1)
                kernels = jnp.concatenate([gr * sr + gi * si, gi * sr - gr * si], 1)
                parts.append(three(jnp.concatenate([adj, conv, kernels], 0), inv_ref, p))
            plus, minus = parts[0] + parts[1], parts[0] - parts[1]
            results = []
            for n in range(3):
                here = slice(n * rows, (n + 1) * rows)
                high, low = split(unturn(plus[here], minus[here], tw_ref))
                results.append(
                    dot(inner_back_ref[...], jnp.concatenate([high, high, low], 0))
                )
            put(ys, c, rows, group, results[0])
            put(ys, c + per_device, rows, group, results[1])
            put(ks.at[s], c, rows, per_device, results[2])
            return carry

        lax.fori_loop(0, per_device, step, 0, unroll=UNROLL)
        for h in range(2):
            lanes = slice(h * HALF, (h + 1) * HALF)
            back[s, :, :, lanes] = ys[h].reshape(pieces, group, HALF).astype(bf16)
            kout[s, :, lanes] = ks[s, h, pl.ds(other, part)].astype(bf16)
        start_exchange(back.at[s], rec_ref.at[s], send_out.at[s], recv_out.at[s])
        peer_copy(kout.at[s], kbuf.at[s], ksend.at[s], krecv.at[s], partner).start()

    for s in range(segments):
        peer_copy(kout.at[s], kbuf.at[s], ksend.at[s], krecv.at[s], partner).wait()
        for h in range(2):
            lanes = slice(h * HALF, (h + 1) * HALF)
            ksum_ref[s, :, lanes] = ks[s, h, pl.ds(own, part)] + kbuf[s, :, lanes].astype(f32)
    for s in range(segments):
        all_of(pack.at[s], recv.at[s], send_in.at[s], recv_in.at[s]).wait_send()
        outgoing = all_of(back.at[s], rec_ref.at[s], send_out.at[s], recv_out.at[s])
        outgoing.wait_send()
        outgoing.wait_recv()


UNROLL = 2


def unpack_kernel(factor, rec_ref, ksum_ref, grad_ref, perm_ref, gs_ref, gg_ref, gf_ref):
    segments, pieces, group, tokens = rec_ref.shape
    per_device = group // 2
    width = pieces * per_device
    for s in range(segments):
        here = slice(s * width, (s + 1) * width)
        rec = rec_ref[s].astype(f32).reshape(pieces * group, tokens).astype(bf16)
        both = dot(rec, perm_ref[...], ((0,), (0,)))
        gs_ref[:, here] = both[:, :width].astype(bf16)
        gg_ref[:, here] = (grad_ref[:, here].astype(f32) * both[:, width:]).astype(bf16)
        for i in range(ksum_ref.shape[1] // per_device):
            gf_ref[s, :, i * U : (i + 1) * U] = (
                ksum_ref[s, i * per_device : (i + 1) * per_device, :] * factor
            )


def vmem(count):
    return [pl.BlockSpec(memory_space=pltpu.VMEM)] * count


def on_device(grad_out, gate, signal, filters):
    tokens, channels = grad_out.shape[1:]
    pieces = lax.axis_size("seq")
    halves = lax.axis_size("dp")
    segments, per_device, length = filters.shape
    group = 2 * per_device
    rows = length * halves // U
    part = length // U * per_device
    tables = [jnp.asarray(t) for t in make_tables(rows)]
    perm = jnp.asarray(make_permutation(pieces, per_device))
    gradient = grad_out[0]
    dma = pltpu.SemaphoreType.DMA
    blocks = (segments, pieces, group, tokens)
    operands = (gradient, gate[0], signal[0], filters, perm, *tables)
    rec, ksum = pl.pallas_call(
        main_kernel,
        out_shape=(
            jax.ShapeDtypeStruct(blocks, bf16),
            jax.ShapeDtypeStruct((segments, part, U), f32),
        ),
        in_specs=[pl.BlockSpec(memory_space=pltpu.HBM)] * 10,
        out_specs=tuple(vmem(2)),
        scratch_shapes=[pltpu.VMEM(x.shape, x.dtype) for x in operands]
        + [
            pltpu.VMEM(blocks, bf16),
            pltpu.VMEM(blocks, bf16),
            pltpu.VMEM(blocks, bf16),
            pltpu.VMEM((segments, part, U), bf16),
            pltpu.VMEM((segments, part, U), bf16),
            pltpu.VMEM((segments, 2, rows * per_device, HALF), f32),
            pltpu.VMEM((segments, 2, rows * per_device, U), f32),
            pltpu.VMEM((2, rows * group, HALF), f32),
            pltpu.VMEM((2, rows * group, HALF), f32),
            pltpu.VMEM((segments, 2, rows * per_device, HALF), f32),
            pltpu.VMEM((segments, part, U), bf16),
            pltpu.VMEM((segments, part, U), bf16),
            dma((segments,)),
            dma((segments,)),
            dma((segments,)),
            dma((segments,)),
            dma,
            dma,
            dma((segments,)),
            dma((segments,)),
            dma((len(operands),)),
        ],
        compiler_params=pltpu.CompilerParams(
            collective_id=0, has_side_effects=True, vmem_limit_bytes=60 << 20
        ),
        name="main",
    )(*operands)
    factor = (halves * rows * U) ** (-0.5)
    grad_signal, grad_gate, grad_filter = pl.pallas_call(
        functools.partial(unpack_kernel, factor),
        out_shape=(
            jax.ShapeDtypeStruct((tokens, channels), bf16),
            jax.ShapeDtypeStruct((tokens, channels), bf16),
            jax.ShapeDtypeStruct(filters.shape, f32),
        ),
        in_specs=vmem(4),
        out_specs=tuple(vmem(3)),
        name="unpack",
    )(rec, ksum, gradient, perm)
    return grad_signal[None], grad_gate[None], grad_filter


def solution(mesh):
    placed = (
        P("dp", "seq", None),
        P("dp", "seq", None),
        P("dp", "seq", None),
        P(None, "seq", "dp"),
    )
    return jax.shard_map(
        on_device,
        mesh=mesh,
        in_specs=placed,
        out_specs=(P("dp", "seq", None), P("dp", "seq", None), P(None, "seq", "dp")),
        check_vma=False,
    )
```

```python
import functools
import math

import jax
import jax.numpy as jnp
import numpy as np
from jax import lax
from jax.experimental import pallas as pl
from jax.experimental.pallas import tpu as pltpu
from jax.sharding import PartitionSpec as P

MESH = pl.DeviceIdType.MESH
bf16 = jnp.bfloat16
f32 = jnp.float32

U = 256
HALF = U // 2


def split_table(table):
    high = jnp.asarray(table, f32).astype(bf16)
    low = (jnp.asarray(table, f32) - high.astype(f32)).astype(bf16)
    return high, low


def np_bf16(table):
    import ml_dtypes

    return np.asarray(table, np.float32).astype(ml_dtypes.bfloat16)


def np_split(table):
    high = np_bf16(table)
    low = np_bf16(np.asarray(table, np.float64) - high.astype(np.float64))
    return high, low


@functools.lru_cache(None)
def make_tables(rows):
    points = 2 * rows * U
    k1 = np.arange(rows)[:, None]
    i = np.arange(rows)[None, :]
    angle = 2 * np.pi * (i * (2 * k1 + 1) % (4 * rows)) / (4 * rows)
    outer = np.concatenate([np.cos(angle), -np.sin(angle)], 0)
    high, low = np_split(outer)
    forward = np.concatenate([high, low, high], 1)
    back_high, back_low = np_split(outer.T * (2.0 / points))
    back = np.concatenate([back_high, back_low, back_high], 1)
    u = np.arange(U)[None, :]
    turn = 2 * np.pi * (u * (2 * k1 + 1)) / (2 * points)
    twiddle = np.stack([np.cos(turn), -np.sin(turn)]).astype(np.float32)
    u0 = np.arange(HALF)[:, None]
    m = np.arange(HALF)[None, :]
    inner = []
    for p in range(2):
        a = 2 * np.pi * (u0 * (2 * m + p) % U) / U
        c, s = np.cos(a), np.sin(a)
        inner.append(np.block([[c, -s], [s, c]]))
    inner = np.stack(inner)
    inner_tables = np.stack(np_split(inner), 1)
    inverse_tables = np.stack(np_split(np.swapaxes(inner, 1, 2)), 1)
    return forward, back, twiddle, inner_tables, inverse_tables


@functools.lru_cache(None)
def make_permutation(pieces, per_device):
    width = pieces * per_device
    row = np.arange(2 * width)
    j, rest = np.divmod(row, 2 * per_device)
    tensor, c = np.divmod(rest, per_device)
    table = np.zeros((2 * width, 2 * width), np.float32)
    table[row, tensor * width + j * per_device + c] = 1
    return np_bf16(table)


def dot(a, b, dims=((1,), (0,))):
    return lax.dot_general(a, b, (dims, ((), ())), preferred_element_type=f32)


def split(x):
    high = x.astype(bf16)
    return high, (x - high.astype(f32)).astype(bf16)


def peer_copy(src_ref, dst_ref, send_sem, recv_sem, peer):
    return pltpu.make_async_remote_copy(
        src_ref=src_ref,
        dst_ref=dst_ref,
        send_sem=send_sem,
        recv_sem=recv_sem,
        device_id=peer,
        device_id_type=MESH,
    )


def for_each_peer(visit):
    me = lax.axis_index("seq")
    far = (2, 3, 1, 0)

    def part(divisor, size):
        return lax.rem(lax.div(me, jnp.int32(divisor)), jnp.int32(size))

    core, x, y, z = part(1, 2), part(2, 4), part(8, 4), part(32, 2)
    low = [
        lax.rem(x + dx, jnp.int32(4)) * 2 + lax.rem(core + dc, jnp.int32(2))
        for dx in far
        for dc in (1, 0)
    ]
    z_other = (1 - z) * 32

    def row(base, targets):
        for target in targets:
            visit(base + target)

    def far_rows(n, carry):
        row(z_other + lax.rem(y + 2 + n, jnp.int32(4)) * 8, low)
        return carry

    def near_rows(n, carry):
        row(z * 32 + lax.rem(y + 1 + n, jnp.int32(4)) * 8, low)
        return carry

    lax.fori_loop(0, 4, far_rows, 0)
    lax.fori_loop(0, 3, near_rows, 0)
    row(z * 32 + y * 8, low[:-1])


def start_exchange(src_ref, dst_ref, send_sem, recv_sem):
    me = lax.axis_index("seq")

    def send(peer):
        peer_copy(
            src_ref.at[peer], dst_ref.at[me], send_sem, recv_sem, {"seq": peer}
        ).start()

    for_each_peer(send)
    dst_ref[me] = src_ref[me]


def all_of(src_ref, dst_ref, send_sem, recv_sem):
    others = pl.ds(0, src_ref.shape[0] - 1)
    return peer_copy(
        src_ref.at[others],
        dst_ref.at[others],
        send_sem,
        recv_sem,
        {"seq": lax.axis_index("seq")},
    )


def greet_all():
    barrier = pltpu.get_barrier_semaphore()

    def greet(peer):
        pl.semaphore_signal(barrier, inc=1, device_id={"seq": peer}, device_id_type=MESH)

    for_each_peer(greet)
    pl.semaphore_signal(
        barrier, inc=1, device_id={"dp": 1 - lax.axis_index("dp")}, device_id_type=MESH
    )
    return barrier


def take(ref, c, rows, stride):
    return jnp.concatenate([ref[h, pl.ds(c, rows, stride=stride), :] for h in range(2)], 1)


def put(ref, c, rows, stride, value):
    for h in range(2):
        ref[h, pl.ds(c, rows, stride=stride), :] = value[:, h * HALF : (h + 1) * HALF]


def turn(p, tw_ref):
    rows = p.shape[0] // 2
    pr, pi = p[:rows], p[rows:]
    tr, ti = tw_ref[0], tw_ref[1]
    qr = pr * tr - pi * ti
    qi = pr * ti + pi * tr
    a = jnp.concatenate([qr[:, :HALF], qi[:, :HALF]], 1)
    b = jnp.concatenate([qr[:, HALF:], qi[:, HALF:]], 1)
    return a + b, a - b


def unturn(plus, minus, tw_ref):
    tr, ti = tw_ref[0], tw_ref[1]
    zr = jnp.concatenate([plus[:, :HALF], minus[:, :HALF]], 1)
    zi = jnp.concatenate([plus[:, HALF:], minus[:, HALF:]], 1)
    return jnp.concatenate([zr * tr + zi * ti, zi * tr - zr * ti], 0)


def three(x, table_ref, p):
    high, low = split(x)
    return dot(high, table_ref[p, 0]) + dot(low, table_ref[p, 0]) + dot(high, table_ref[p, 1])


def main_kernel(*refs):
    operands, refs = refs[:10], refs[10:]
    rec_ref, ksum_ref = refs[:2]
    held, refs = refs[2:12], refs[12:]
    grad_ref, gate_ref, signal_ref, filters_ref, perm_ref = held[:5]
    fwd_ref, inner_back_ref, tw_ref, in_ref, inv_ref = held[5:]
    pack, recv, back, pf, pfin, fs, fspec, xs, ys, ks, kout, kbuf = refs[:12]
    send_in, recv_in, send_out, recv_out, fsend, frecv, ksend, krecv, load_sem = refs[12:]
    segments, pieces, group, tokens = pack.shape
    per_device = group // 2
    rows = pieces * tokens // U
    part = pf.shape[1]
    dp = lax.axis_index("dp")
    partner = {"dp": 1 - dp}
    loads = [
        pltpu.make_async_copy(operands[n], held[n], load_sem.at[n]) for n in range(len(held))
    ]
    for n in (3, 0, 1, 2, 4, 5, 6, 7, 8, 9):
        loads[n].start()
    barrier = greet_all()

    loads[3].wait()
    own = dp * part
    other = (1 - dp) * part
    for s in range(segments):
        for i in range(part // per_device):
            for h in range(2):
                fs[s, h, pl.ds(own + i * per_device, per_device), :] = filters_ref[
                    s, :, i * U + h * HALF : i * U + (h + 1) * HALF
                ]
        for h in range(2):
            pf[s, :, h * HALF : (h + 1) * HALF] = fs[s, h, pl.ds(own, part)].astype(bf16)
    for n in (0, 1, 2, 4):
        loads[n].wait()
    width = pieces * per_device
    for s in range(segments):
        here = slice(s * width, (s + 1) * width)
        scaled = (grad_ref[:, here].astype(f32) * gate_ref[:, here].astype(f32)).astype(bf16)
        joined = jnp.concatenate([scaled, signal_ref[:, here]], 1)
        moved = dot(perm_ref[...], joined, ((1,), (1,)))
        pack[s] = moved.reshape(pieces, group, tokens).astype(bf16)

    pl.semaphore_wait(barrier, pieces)
    filter_copy = peer_copy(pf, pfin, fsend, frecv, partner)
    filter_copy.start()
    for s in range(segments):
        start_exchange(pack.at[s], recv.at[s], send_in.at[s], recv_in.at[s])
    for n in range(5, 10):
        loads[n].wait()
    filter_copy.wait()
    for h in range(2):
        lanes = slice(h * HALF, (h + 1) * HALF)
        for s in range(segments):
            fs[s, h, pl.ds(other, part)] = pfin[s, :, lanes].astype(f32)

    for s in range(segments):

        def filter_step(n, carry, s=s):
            stages = []
            for c in (2 * n, 2 * n + 1):
                high, low = split(take(fs.at[s], c, rows, per_device))
                stages.append(
                    turn(dot(fwd_ref[...], jnp.concatenate([high, high, low], 0)), tw_ref)
                )
            at = pl.multiple_of(n * 2 * rows, 2 * rows)
            for p in range(2):
                fspec[s, p, pl.ds(at, 2 * rows)] = three(
                    jnp.concatenate([t[p] for t in stages], 0), in_ref, p
                )
            return carry

        lax.fori_loop(0, per_device // 2, filter_step, 0)

    short = fwd_ref[:, : 2 * rows]
    for s in range(segments):
        incoming = all_of(pack.at[s], recv.at[s], send_in.at[s], recv_in.at[s])
        incoming.wait_recv()
        for h in range(2):
            lanes = slice(h * HALF, (h + 1) * HALF)
            xs[h] = recv[s, :, :, lanes].astype(f32).reshape(rows * group, HALF)

        def step(n, carry, s=s):
            channels = [n * BATCHED + k for k in range(BATCHED)]
            turned = []
            for c in channels:
                for r in (c, c + per_device):
                    x = take(xs, r, rows, group).astype(bf16)
                    turned.append(turn(dot(short, jnp.concatenate([x, x], 0)), tw_ref))
            parts = []
            for p in range(2):
                spec = three(jnp.concatenate([t[p] for t in turned], 0), in_ref, p)
                products = []
                for k, c in enumerate(channels):
                    at = pl.multiple_of(c * rows, rows)
                    fr = fspec[s, p, pl.ds(at, rows), :HALF]
                    fi = fspec[s, p, pl.ds(at, rows), HALF:]
                    g = spec[2 * k * rows : (2 * k + 1) * rows]
                    x = spec[(2 * k + 1) * rows : (2 * k + 2) * rows]
                    gr, gi, sr, si = g[:, :HALF], g[:, HALF:], x[:, :HALF], x[:, HALF:]
                    products += [
                        jnp.concatenate([fr * gr + fi * gi, fr * gi - fi * gr], 1),
                        jnp.concatenate([fr * sr - fi * si, fr * si + fi * sr], 1),
                        jnp.concatenate([gr * sr + gi * si, gi * sr - gr * si], 1),
                    ]
                parts.append(three(jnp.concatenate(products, 0), inv_ref, p))
            plus, minus = parts[0] + parts[1], parts[0] - parts[1]
            for k, c in enumerate(channels):
                results = []
                for m in range(3):
                    here = slice((3 * k + m) * rows, (3 * k + m + 1) * rows)
                    high, low = split(unturn(plus[here], minus[here], tw_ref))
                    results.append(
                        dot(inner_back_ref[...], jnp.concatenate([high, high, low], 0))
                    )
                put(ys, c, rows, group, results[0])
                put(ys, c + per_device, rows, group, results[1])
                put(ks.at[s], c, rows, per_device, results[2])
            return carry

        lax.fori_loop(0, per_device // BATCHED, step, 0, unroll=UNROLL)
        for h in range(2):
            lanes = slice(h * HALF, (h + 1) * HALF)
            back[s, :, :, lanes] = ys[h].reshape(pieces, group, HALF).astype(bf16)
            kout[s, :, lanes] = ks[s, h, pl.ds(other, part)].astype(bf16)
        start_exchange(back.at[s], rec_ref.at[s], send_out.at[s], recv_out.at[s])
        peer_copy(kout.at[s], kbuf.at[s], ksend.at[s], krecv.at[s], partner).start()

    for s in range(segments):
        peer_copy(kout.at[s], kbuf.at[s], ksend.at[s], krecv.at[s], partner).wait()
        for h in range(2):
            lanes = slice(h * HALF, (h + 1) * HALF)
            ksum_ref[s, :, lanes] = ks[s, h, pl.ds(own, part)] + kbuf[s, :, lanes].astype(f32)
    for s in range(segments):
        all_of(pack.at[s], recv.at[s], send_in.at[s], recv_in.at[s]).wait_send()
        outgoing = all_of(back.at[s], rec_ref.at[s], send_out.at[s], recv_out.at[s])
        outgoing.wait_send()
        outgoing.wait_recv()


UNROLL = 1
BATCHED = 4


def unpack_kernel(factor, rec_ref, ksum_ref, grad_ref, perm_ref, gs_ref, gg_ref, gf_ref):
    segments, pieces, group, tokens = rec_ref.shape
    per_device = group // 2
    width = pieces * per_device
    for s in range(segments):
        here = slice(s * width, (s + 1) * width)
        rec = rec_ref[s].astype(f32).reshape(pieces * group, tokens).astype(bf16)
        both = dot(rec, perm_ref[...], ((0,), (0,)))
        gs_ref[:, here] = both[:, :width].astype(bf16)
        gg_ref[:, here] = (grad_ref[:, here].astype(f32) * both[:, width:]).astype(bf16)
        for i in range(ksum_ref.shape[1] // per_device):
            gf_ref[s, :, i * U : (i + 1) * U] = (
                ksum_ref[s, i * per_device : (i + 1) * per_device, :] * factor
            )


def vmem(count):
    return [pl.BlockSpec(memory_space=pltpu.VMEM)] * count


def on_device(grad_out, gate, signal, filters):
    tokens, channels = grad_out.shape[1:]
    pieces = lax.axis_size("seq")
    halves = lax.axis_size("dp")
    segments, per_device, length = filters.shape
    group = 2 * per_device
    rows = length * halves // U
    part = length // U * per_device
    tables = [jnp.asarray(t) for t in make_tables(rows)]
    perm = jnp.asarray(make_permutation(pieces, per_device))
    gradient = grad_out[0]
    dma = pltpu.SemaphoreType.DMA
    blocks = (segments, pieces, group, tokens)
    operands = (gradient, gate[0], signal[0], filters, perm, *tables)
    rec, ksum = pl.pallas_call(
        main_kernel,
        out_shape=(
            jax.ShapeDtypeStruct(blocks, bf16),
            jax.ShapeDtypeStruct((segments, part, U), f32),
        ),
        in_specs=[pl.BlockSpec(memory_space=pltpu.HBM)] * 10,
        out_specs=tuple(vmem(2)),
        scratch_shapes=[pltpu.VMEM(x.shape, x.dtype) for x in operands]
        + [
            pltpu.VMEM(blocks, bf16),
            pltpu.VMEM(blocks, bf16),
            pltpu.VMEM(blocks, bf16),
            pltpu.VMEM((segments, part, U), bf16),
            pltpu.VMEM((segments, part, U), bf16),
            pltpu.VMEM((segments, 2, rows * per_device, HALF), f32),
            pltpu.VMEM((segments, 2, rows * per_device, U), f32),
            pltpu.VMEM((2, rows * group, HALF), f32),
            pltpu.VMEM((2, rows * group, HALF), f32),
            pltpu.VMEM((segments, 2, rows * per_device, HALF), f32),
            pltpu.VMEM((segments, part, U), bf16),
            pltpu.VMEM((segments, part, U), bf16),
            dma((segments,)),
            dma((segments,)),
            dma((segments,)),
            dma((segments,)),
            dma,
            dma,
            dma((segments,)),
            dma((segments,)),
            dma((len(operands),)),
        ],
        compiler_params=pltpu.CompilerParams(
            collective_id=0, has_side_effects=True, vmem_limit_bytes=60 << 20
        ),
        name="main",
    )(*operands)
    factor = (halves * rows * U) ** (-0.5)
    grad_signal, grad_gate, grad_filter = pl.pallas_call(
        functools.partial(unpack_kernel, factor),
        out_shape=(
            jax.ShapeDtypeStruct((tokens, channels), bf16),
            jax.ShapeDtypeStruct((tokens, channels), bf16),
            jax.ShapeDtypeStruct(filters.shape, f32),
        ),
        in_specs=vmem(4),
        out_specs=tuple(vmem(3)),
        name="unpack",
    )(rec, ksum, gradient, perm)
    return grad_signal[None], grad_gate[None], grad_filter


def solution(mesh):
    placed = (
        P("dp", "seq", None),
        P("dp", "seq", None),
        P("dp", "seq", None),
        P(None, "seq", "dp"),
    )
    return jax.shard_map(
        on_device,
        mesh=mesh,
        in_specs=placed,
        out_specs=(P("dp", "seq", None), P("dp", "seq", None), P(None, "seq", "dp")),
        check_vma=False,
    )
```

```python
import functools
import math

import jax
import jax.numpy as jnp
import numpy as np
from jax import lax
from jax.experimental import pallas as pl
from jax.experimental.pallas import tpu as pltpu
from jax.sharding import PartitionSpec as P

MESH = pl.DeviceIdType.MESH
bf16 = jnp.bfloat16
f32 = jnp.float32

U = 256
HALF = U // 2


def split_table(table):
    high = jnp.asarray(table, f32).astype(bf16)
    low = (jnp.asarray(table, f32) - high.astype(f32)).astype(bf16)
    return high, low


def np_bf16(table):
    import ml_dtypes

    return np.asarray(table, np.float32).astype(ml_dtypes.bfloat16)


def np_split(table):
    high = np_bf16(table)
    low = np_bf16(np.asarray(table, np.float64) - high.astype(np.float64))
    return high, low


@functools.lru_cache(None)
def make_tables(rows):
    points = 2 * rows * U
    k1 = np.arange(rows)[:, None]
    i = np.arange(rows)[None, :]
    angle = 2 * np.pi * (i * (2 * k1 + 1) % (4 * rows)) / (4 * rows)
    outer = np.concatenate([np.cos(angle), -np.sin(angle)], 0)
    high, low = np_split(outer)
    forward = np.concatenate([high, low, high], 1)
    back_high, back_low = np_split(outer.T * (2.0 / points))
    back = np.concatenate([back_high, back_low, back_high], 1)
    u = np.arange(U)[None, :]
    turn = 2 * np.pi * (u * (2 * k1 + 1)) / (2 * points)
    twiddle = np.stack([np.cos(turn), -np.sin(turn)]).astype(np.float32)
    u0 = np.arange(HALF)[:, None]
    m = np.arange(HALF)[None, :]
    inner = []
    for p in range(2):
        a = 2 * np.pi * (u0 * (2 * m + p) % U) / U
        c, s = np.cos(a), np.sin(a)
        inner.append(np.block([[c, -s], [s, c]]))
    inner = np.stack(inner)
    inner_tables = np.stack(np_split(inner), 1)
    inverse_tables = np.stack(np_split(np.swapaxes(inner, 1, 2)), 1)
    return forward, back, twiddle, inner_tables, inverse_tables


@functools.lru_cache(None)
def make_permutation(pieces, per_device):
    width = pieces * per_device
    row = np.arange(2 * width)
    j, rest = np.divmod(row, 2 * per_device)
    tensor, c = np.divmod(rest, per_device)
    table = np.zeros((2 * width, 2 * width), np.float32)
    table[row, tensor * width + j * per_device + c] = 1
    return np_bf16(table)


def dot(a, b, dims=((1,), (0,))):
    return lax.dot_general(a, b, (dims, ((), ())), preferred_element_type=f32)


def split(x):
    high = x.astype(bf16)
    return high, (x - high.astype(f32)).astype(bf16)


def peer_copy(src_ref, dst_ref, send_sem, recv_sem, peer):
    return pltpu.make_async_remote_copy(
        src_ref=src_ref,
        dst_ref=dst_ref,
        send_sem=send_sem,
        recv_sem=recv_sem,
        device_id=peer,
        device_id_type=MESH,
    )


def for_each_peer(visit):
    me = lax.axis_index("seq")
    far = (2, 3, 1, 0)

    def part(divisor, size):
        return lax.rem(lax.div(me, jnp.int32(divisor)), jnp.int32(size))

    core, x, y, z = part(1, 2), part(2, 4), part(8, 4), part(32, 2)
    low = [
        lax.rem(x + dx, jnp.int32(4)) * 2 + lax.rem(core + dc, jnp.int32(2))
        for dx in far
        for dc in (1, 0)
    ]
    z_other = (1 - z) * 32

    def row(base, targets):
        for target in targets:
            visit(base + target)

    def far_rows(n, carry):
        row(z_other + lax.rem(y + 2 + n, jnp.int32(4)) * 8, low)
        return carry

    def near_rows(n, carry):
        row(z * 32 + lax.rem(y + 1 + n, jnp.int32(4)) * 8, low)
        return carry

    lax.fori_loop(0, 4, far_rows, 0)
    lax.fori_loop(0, 3, near_rows, 0)
    row(z * 32 + y * 8, low[:-1])


def start_exchange(src_ref, dst_ref, send_sem, recv_sem):
    me = lax.axis_index("seq")

    def send(peer):
        peer_copy(
            src_ref.at[peer], dst_ref.at[me], send_sem, recv_sem, {"seq": peer}
        ).start()

    for_each_peer(send)
    dst_ref[me] = src_ref[me]


def all_of(src_ref, dst_ref, send_sem, recv_sem):
    others = pl.ds(0, src_ref.shape[0] - 1)
    return peer_copy(
        src_ref.at[others],
        dst_ref.at[others],
        send_sem,
        recv_sem,
        {"seq": lax.axis_index("seq")},
    )


def greet_all():
    barrier = pltpu.get_barrier_semaphore()

    def greet(peer):
        pl.semaphore_signal(barrier, inc=1, device_id={"seq": peer}, device_id_type=MESH)

    for_each_peer(greet)
    pl.semaphore_signal(
        barrier, inc=1, device_id={"dp": 1 - lax.axis_index("dp")}, device_id_type=MESH
    )
    return barrier


def take(ref, c, rows, stride):
    return jnp.concatenate([ref[h, pl.ds(c, rows, stride=stride), :] for h in range(2)], 1)


def put(ref, c, rows, stride, value):
    for h in range(2):
        ref[h, pl.ds(c, rows, stride=stride), :] = value[:, h * HALF : (h + 1) * HALF]


def turn(p, tw_ref):
    rows = p.shape[0] // 2
    pr, pi = p[:rows], p[rows:]
    tr, ti = tw_ref[0], tw_ref[1]
    qr = pr * tr - pi * ti
    qi = pr * ti + pi * tr
    a = jnp.concatenate([qr[:, :HALF], qi[:, :HALF]], 1)
    b = jnp.concatenate([qr[:, HALF:], qi[:, HALF:]], 1)
    return a + b, a - b


def unturn(plus, minus, tw_ref):
    tr, ti = tw_ref[0], tw_ref[1]
    zr = jnp.concatenate([plus[:, :HALF], minus[:, :HALF]], 1)
    zi = jnp.concatenate([plus[:, HALF:], minus[:, HALF:]], 1)
    return jnp.concatenate([zr * tr + zi * ti, zi * tr - zr * ti], 0)


def three(x, table_ref, p):
    high, low = split(x)
    return dot(high, table_ref[p, 0]) + dot(low, table_ref[p, 0]) + dot(high, table_ref[p, 1])


def main_kernel(factor, *refs):
    operands, refs = refs[:10], refs[10:]
    outs, refs = refs[:3], refs[3:]
    held, refs = refs[:10], refs[10:]
    grad_ref, gate_ref, signal_ref, filters_ref, perm_ref = held[:5]
    fwd_ref, inner_back_ref, tw_ref, in_ref, inv_ref = held[5:]
    pack, recv, back, rec, pf, pfin, fs, fspec, xs, ys, ks, ksum, kout, kbuf = refs[:14]
    made, refs = refs[14:17], refs[17:]
    gs, gg, gf = made
    send_in, recv_in, send_out, recv_out, fsend, frecv, ksend, krecv, load_sem, store_sem = refs
    segments, pieces, group, tokens = pack.shape
    per_device = group // 2
    rows = pieces * tokens // U
    part = pf.shape[1]
    dp = lax.axis_index("dp")
    partner = {"dp": 1 - dp}
    loads = [
        pltpu.make_async_copy(operands[n], held[n], load_sem.at[n]) for n in range(len(held))
    ]
    for n in (3, 0, 1, 2, 4, 5, 6, 7, 8, 9):
        loads[n].start()
    barrier = greet_all()

    loads[3].wait()
    own = dp * part
    other = (1 - dp) * part
    for s in range(segments):
        for i in range(part // per_device):
            for h in range(2):
                fs[s, h, pl.ds(own + i * per_device, per_device), :] = filters_ref[
                    s, :, i * U + h * HALF : i * U + (h + 1) * HALF
                ]
        for h in range(2):
            pf[s, :, h * HALF : (h + 1) * HALF] = fs[s, h, pl.ds(own, part)].astype(bf16)
    for n in (0, 1, 2, 4):
        loads[n].wait()
    width = pieces * per_device
    for s in range(segments):
        here = slice(s * width, (s + 1) * width)
        scaled = (grad_ref[:, here].astype(f32) * gate_ref[:, here].astype(f32)).astype(bf16)
        joined = jnp.concatenate([scaled, signal_ref[:, here]], 1)
        moved = dot(perm_ref[...], joined, ((1,), (1,)))
        pack[s] = moved.reshape(pieces, group, tokens).astype(bf16)

    pl.semaphore_wait(barrier, pieces)
    filter_copy = peer_copy(pf, pfin, fsend, frecv, partner)
    filter_copy.start()
    for s in range(segments):
        start_exchange(pack.at[s], recv.at[s], send_in.at[s], recv_in.at[s])
    for n in range(5, 10):
        loads[n].wait()
    filter_copy.wait()
    for h in range(2):
        lanes = slice(h * HALF, (h + 1) * HALF)
        for s in range(segments):
            fs[s, h, pl.ds(other, part)] = pfin[s, :, lanes].astype(f32)

    for s in range(segments):

        def filter_step(n, carry, s=s):
            stages = []
            for c in (2 * n, 2 * n + 1):
                high, low = split(take(fs.at[s], c, rows, per_device))
                stages.append(
                    turn(dot(fwd_ref[...], jnp.concatenate([high, high, low], 0)), tw_ref)
                )
            at = pl.multiple_of(n * 2 * rows, 2 * rows)
            for p in range(2):
                fspec[s, p, pl.ds(at, 2 * rows)] = three(
                    jnp.concatenate([t[p] for t in stages], 0), in_ref, p
                )
            return carry

        lax.fori_loop(0, per_device // 2, filter_step, 0)

    short = fwd_ref[:, : 2 * rows]
    for s in range(segments):
        incoming = all_of(pack.at[s], recv.at[s], send_in.at[s], recv_in.at[s])
        incoming.wait_recv()
        for h in range(2):
            lanes = slice(h * HALF, (h + 1) * HALF)
            xs[h] = recv[s, :, :, lanes].astype(f32).reshape(rows * group, HALF)

        def step(n, carry, s=s):
            channels = [n * BATCHED + k for k in range(BATCHED)]
            turned = []
            for c in channels:
                for r in (c, c + per_device):
                    x = take(xs, r, rows, group).astype(bf16)
                    turned.append(turn(dot(short, jnp.concatenate([x, x], 0)), tw_ref))
            parts = []
            for p in range(2):
                spec = three(jnp.concatenate([t[p] for t in turned], 0), in_ref, p)
                products = []
                for k, c in enumerate(channels):
                    at = pl.multiple_of(c * rows, rows)
                    fr = fspec[s, p, pl.ds(at, rows), :HALF]
                    fi = fspec[s, p, pl.ds(at, rows), HALF:]
                    g = spec[2 * k * rows : (2 * k + 1) * rows]
                    x = spec[(2 * k + 1) * rows : (2 * k + 2) * rows]
                    gr, gi, sr, si = g[:, :HALF], g[:, HALF:], x[:, :HALF], x[:, HALF:]
                    products += [
                        jnp.concatenate([fr * gr + fi * gi, fr * gi - fi * gr], 1),
                        jnp.concatenate([fr * sr - fi * si, fr * si + fi * sr], 1),
                        jnp.concatenate([gr * sr + gi * si, gi * sr - gr * si], 1),
                    ]
                parts.append(three(jnp.concatenate(products, 0), inv_ref, p))
            plus, minus = parts[0] + parts[1], parts[0] - parts[1]
            for k, c in enumerate(channels):
                results = []
                for m in range(3):
                    here = slice((3 * k + m) * rows, (3 * k + m + 1) * rows)
                    high, low = split(unturn(plus[here], minus[here], tw_ref))
                    results.append(
                        dot(inner_back_ref[...], jnp.concatenate([high, high, low], 0))
                    )
                put(ys, c, rows, group, results[0])
                put(ys, c + per_device, rows, group, results[1])
                put(ks.at[s], c, rows, per_device, results[2])
            return carry

        lax.fori_loop(0, per_device // BATCHED, step, 0, unroll=UNROLL)
        for h in range(2):
            lanes = slice(h * HALF, (h + 1) * HALF)
            back[s, :, :, lanes] = ys[h].reshape(pieces, group, HALF).astype(bf16)
            kout[s, :, lanes] = ks[s, h, pl.ds(other, part)].astype(bf16)
        start_exchange(back.at[s], rec.at[s], send_out.at[s], recv_out.at[s])
        peer_copy(kout.at[s], kbuf.at[s], ksend.at[s], krecv.at[s], partner).start()

    stores = []

    def store(n, s, at):
        copy = pltpu.make_async_copy(made[n].at[at], outs[n].at[at], store_sem.at[n, s])
        copy.start()
        stores.append(copy)

    for s in range(segments):
        peer_copy(kout.at[s], kbuf.at[s], ksend.at[s], krecv.at[s], partner).wait()
        for h in range(2):
            lanes = slice(h * HALF, (h + 1) * HALF)
            mine = ks[s, h, pl.ds(own, part)]
            ksum[h] = (mine + kbuf[s, :, lanes].astype(f32)) * factor
            for i in range(part // per_device):
                gf[s, :, i * U + h * HALF : i * U + (h + 1) * HALF] = ksum[
                    h, i * per_device : (i + 1) * per_device, :
                ]
        store(2, s, (s,))
        all_of(back.at[s], rec.at[s], send_out.at[s], recv_out.at[s]).wait_recv()
        here = slice(s * width, (s + 1) * width)
        arrived = rec[s].astype(f32).reshape(pieces * group, tokens).astype(bf16)
        both = dot(arrived, perm_ref[...], ((0,), (0,)))
        gs[:, here] = both[:, :width].astype(bf16)
        gg[:, here] = (grad_ref[:, here].astype(f32) * both[:, width:]).astype(bf16)
        at = (slice(None), pl.ds(s * width, width))
        store(0, s, at)
        store(1, s, at)
    for s in range(segments):
        all_of(pack.at[s], recv.at[s], send_in.at[s], recv_in.at[s]).wait_send()
        all_of(back.at[s], rec.at[s], send_out.at[s], recv_out.at[s]).wait_send()
    for copy in stores:
        copy.wait()


UNROLL = 1
BATCHED = 4


def finish_kernel(*refs):
    sources, outs, held = refs[:3], refs[3:6], refs[6:9]
    sems = refs[9]
    loads = [pltpu.make_async_copy(sources[n], held[n], sems.at[0, n]) for n in range(3)]
    stores = [pltpu.make_async_copy(held[n], outs[n], sems.at[1, n]) for n in range(3)]
    for copy in loads:
        copy.start()
    for n in range(3):
        loads[n].wait()
        stores[n].start()
    for copy in stores:
        copy.wait()


def hbm(count):
    return [pl.BlockSpec(memory_space=pltpu.HBM)] * count


def on_device(grad_out, gate, signal, filters):
    tokens, channels = grad_out.shape[1:]
    pieces = lax.axis_size("seq")
    halves = lax.axis_size("dp")
    segments, per_device, length = filters.shape
    group = 2 * per_device
    rows = length * halves // U
    part = length // U * per_device
    tables = [jnp.asarray(t) for t in make_tables(rows)]
    perm = jnp.asarray(make_permutation(pieces, per_device))
    gradient = grad_out[0]
    dma = pltpu.SemaphoreType.DMA
    blocks = (segments, pieces, group, tokens)
    operands = (gradient, gate[0], signal[0], filters, perm, *tables)
    factor = (halves * rows * U) ** (-0.5)
    results = (
        jax.ShapeDtypeStruct((tokens, channels), bf16),
        jax.ShapeDtypeStruct((tokens, channels), bf16),
        jax.ShapeDtypeStruct(filters.shape, f32),
    )
    made = pl.pallas_call(
        functools.partial(main_kernel, factor),
        out_shape=results,
        in_specs=hbm(10),
        out_specs=tuple(hbm(3)),
        scratch_shapes=[pltpu.VMEM(x.shape, x.dtype) for x in operands]
        + [
            pltpu.VMEM(blocks, bf16),
            pltpu.VMEM(blocks, bf16),
            pltpu.VMEM(blocks, bf16),
            pltpu.VMEM(blocks, bf16),
            pltpu.VMEM((segments, part, U), bf16),
            pltpu.VMEM((segments, part, U), bf16),
            pltpu.VMEM((segments, 2, rows * per_device, HALF), f32),
            pltpu.VMEM((segments, 2, rows * per_device, U), f32),
            pltpu.VMEM((2, rows * group, HALF), f32),
            pltpu.VMEM((2, rows * group, HALF), f32),
            pltpu.VMEM((segments, 2, rows * per_device, HALF), f32),
            pltpu.VMEM((2, part, HALF), f32),
            pltpu.VMEM((segments, part, U), bf16),
            pltpu.VMEM((segments, part, U), bf16),
            *[pltpu.VMEM(x.shape, x.dtype) for x in results],
            dma((segments,)),
            dma((segments,)),
            dma((segments,)),
            dma((segments,)),
            dma,
            dma,
            dma((segments,)),
            dma((segments,)),
            dma((len(operands),)),
            dma((3, segments)),
        ],
        compiler_params=pltpu.CompilerParams(
            collective_id=0, has_side_effects=True, vmem_limit_bytes=60 << 20
        ),
        name="main",
    )(*operands)
    grad_signal, grad_gate, grad_filter = pl.pallas_call(
        finish_kernel,
        out_shape=results,
        in_specs=hbm(3),
        out_specs=tuple(hbm(3)),
        scratch_shapes=[pltpu.VMEM(x.shape, x.dtype) for x in results] + [dma((2, 3))],
        name="finish",
    )(*made)
    return grad_signal[None], grad_gate[None], grad_filter


def solution(mesh):
    placed = (
        P("dp", "seq", None),
        P("dp", "seq", None),
        P("dp", "seq", None),
        P(None, "seq", "dp"),
    )
    return jax.shard_map(
        on_device,
        mesh=mesh,
        in_specs=placed,
        out_specs=(P("dp", "seq", None), P("dp", "seq", None), P(None, "seq", "dp")),
        check_vma=False,
    )
```

```python
import functools
import math

import jax
import jax.numpy as jnp
import numpy as np
from jax import lax
from jax.experimental import pallas as pl
from jax.experimental.pallas import tpu as pltpu
from jax.sharding import PartitionSpec as P

MESH = pl.DeviceIdType.MESH
bf16 = jnp.bfloat16
f32 = jnp.float32

U = 256
HALF = U // 2


def split_table(table):
    high = jnp.asarray(table, f32).astype(bf16)
    low = (jnp.asarray(table, f32) - high.astype(f32)).astype(bf16)
    return high, low


def np_bf16(table):
    import ml_dtypes

    return np.asarray(table, np.float32).astype(ml_dtypes.bfloat16)


def np_split(table):
    high = np_bf16(table)
    low = np_bf16(np.asarray(table, np.float64) - high.astype(np.float64))
    return high, low


@functools.lru_cache(None)
def make_tables(rows):
    points = 2 * rows * U
    k1 = np.arange(rows)[:, None]
    i = np.arange(rows)[None, :]
    angle = 2 * np.pi * (i * (2 * k1 + 1) % (4 * rows)) / (4 * rows)
    outer = np.concatenate([np.cos(angle), -np.sin(angle)], 0)
    high, low = np_split(outer)
    forward = np.concatenate([high, low, high], 1)
    back_high, back_low = np_split(outer.T * (2.0 / points))
    back = np.concatenate([back_high, back_low, back_high], 1)
    u = np.arange(U)[None, :]
    turn = 2 * np.pi * (u * (2 * k1 + 1)) / (2 * points)
    twiddle = np.stack([np.cos(turn), -np.sin(turn)]).astype(np.float32)
    u0 = np.arange(HALF)[:, None]
    m = np.arange(HALF)[None, :]
    inner = []
    for p in range(2):
        a = 2 * np.pi * (u0 * (2 * m + p) % U) / U
        c, s = np.cos(a), np.sin(a)
        inner.append(np.block([[c, -s], [s, c]]))
    inner = np.stack(inner)
    inner_tables = np.stack(np_split(inner), 1)
    inverse_tables = np.stack(np_split(np.swapaxes(inner, 1, 2)), 1)
    return forward, back, twiddle, inner_tables, inverse_tables


@functools.lru_cache(None)
def make_permutation(pieces, per_device):
    width = pieces * per_device
    row = np.arange(2 * width)
    j, rest = np.divmod(row, 2 * per_device)
    tensor, c = np.divmod(rest, per_device)
    table = np.zeros((2 * width, 2 * width), np.float32)
    table[row, tensor * width + j * per_device + c] = 1
    return np_bf16(table)


def dot(a, b, dims=((1,), (0,))):
    return lax.dot_general(a, b, (dims, ((), ())), preferred_element_type=f32)


def split(x):
    high = x.astype(bf16)
    return high, (x - high.astype(f32)).astype(bf16)


def peer_copy(src_ref, dst_ref, send_sem, recv_sem, peer):
    return pltpu.make_async_remote_copy(
        src_ref=src_ref,
        dst_ref=dst_ref,
        send_sem=send_sem,
        recv_sem=recv_sem,
        device_id=peer,
        device_id_type=MESH,
    )


def for_each_peer(visit):
    me = lax.axis_index("seq")
    far = (2, 3, 1, 0)

    def part(divisor, size):
        return lax.rem(lax.div(me, jnp.int32(divisor)), jnp.int32(size))

    core, x, y, z = part(1, 2), part(2, 4), part(8, 4), part(32, 2)
    low = [
        lax.rem(x + dx, jnp.int32(4)) * 2 + lax.rem(core + dc, jnp.int32(2))
        for dx in far
        for dc in (1, 0)
    ]
    z_other = (1 - z) * 32

    def row(base, targets):
        for target in targets:
            visit(base + target)

    def far_rows(n, carry):
        row(z_other + lax.rem(y + 2 + n, jnp.int32(4)) * 8, low)
        return carry

    def near_rows(n, carry):
        row(z * 32 + lax.rem(y + 1 + n, jnp.int32(4)) * 8, low)
        return carry

    lax.fori_loop(0, 4, far_rows, 0)
    lax.fori_loop(0, 3, near_rows, 0)
    row(z * 32 + y * 8, low[:-1])


def start_exchange(src_ref, dst_ref, send_sem, recv_sem):
    me = lax.axis_index("seq")

    def send(peer):
        peer_copy(
            src_ref.at[peer], dst_ref.at[me], send_sem, recv_sem, {"seq": peer}
        ).start()

    for_each_peer(send)
    dst_ref[me] = src_ref[me]


def all_of(src_ref, dst_ref, send_sem, recv_sem):
    others = pl.ds(0, src_ref.shape[0] - 1)
    return peer_copy(
        src_ref.at[others],
        dst_ref.at[others],
        send_sem,
        recv_sem,
        {"seq": lax.axis_index("seq")},
    )


def greet_all():
    barrier = pltpu.get_barrier_semaphore()

    def greet(peer):
        pl.semaphore_signal(barrier, inc=1, device_id={"seq": peer}, device_id_type=MESH)

    for_each_peer(greet)
    pl.semaphore_signal(
        barrier, inc=1, device_id={"dp": 1 - lax.axis_index("dp")}, device_id_type=MESH
    )
    return barrier


def take(ref, c, rows, stride):
    return jnp.concatenate([ref[h, pl.ds(c, rows, stride=stride), :] for h in range(2)], 1)


def put(ref, c, rows, stride, value):
    for h in range(2):
        ref[h, pl.ds(c, rows, stride=stride), :] = value[:, h * HALF : (h + 1) * HALF]


def turn(p, tw_ref):
    rows = p.shape[0] // 2
    pr, pi = p[:rows], p[rows:]
    tr, ti = tw_ref[0], tw_ref[1]
    qr = pr * tr - pi * ti
    qi = pr * ti + pi * tr
    a = jnp.concatenate([qr[:, :HALF], qi[:, :HALF]], 1)
    b = jnp.concatenate([qr[:, HALF:], qi[:, HALF:]], 1)
    return a + b, a - b


def unturn(plus, minus, tw_ref):
    tr, ti = tw_ref[0], tw_ref[1]
    zr = jnp.concatenate([plus[:, :HALF], minus[:, :HALF]], 1)
    zi = jnp.concatenate([plus[:, HALF:], minus[:, HALF:]], 1)
    return jnp.concatenate([zr * tr + zi * ti, zi * tr - zr * ti], 0)


def three(x, table_ref, p):
    high, low = split(x)
    return dot(high, table_ref[p, 0]) + dot(low, table_ref[p, 0]) + dot(high, table_ref[p, 1])


def main_kernel(factor, *refs):
    operands, refs = refs[:10], refs[10:]
    outs, refs = refs[:3], refs[3:]
    held, refs = refs[:10], refs[10:]
    grad_ref, gate_ref, signal_ref, filters_ref, perm_ref = held[:5]
    fwd_ref, inner_back_ref, tw_ref, in_ref, inv_ref = held[5:]
    pack, recv, back, rec, pf, pfin, fs, fspec, xs, ys, ks, ksum, kout, kbuf = refs[:14]
    made, refs = refs[14:17], refs[17:]
    gs, gg, gf = made
    send_in, recv_in, send_out, recv_out, fsend, frecv, ksend, krecv, load_sem, store_sem = refs
    segments, pieces, group, tokens = pack.shape
    per_device = group // 2
    rows = pieces * tokens // U
    part = pf.shape[1]
    dp = lax.axis_index("dp")
    partner = {"dp": 1 - dp}
    loads = [
        pltpu.make_async_copy(operands[n], held[n], load_sem.at[n]) for n in range(len(held))
    ]
    for n in (3, 0, 1, 2, 4, 5, 6, 7, 8, 9):
        loads[n].start()
    barrier = greet_all()

    loads[3].wait()
    own = dp * part
    other = (1 - dp) * part
    for s in range(segments):
        for i in range(part // per_device):
            for h in range(2):
                fs[s, h, pl.ds(own + i * per_device, per_device), :] = filters_ref[
                    s, :, i * U + h * HALF : i * U + (h + 1) * HALF
                ]
        for h in range(2):
            pf[s, :, h * HALF : (h + 1) * HALF] = fs[s, h, pl.ds(own, part)].astype(bf16)
    for n in (0, 1, 2, 4):
        loads[n].wait()
    width = pieces * per_device
    for s in range(segments):
        here = slice(s * width, (s + 1) * width)
        scaled = (grad_ref[:, here].astype(f32) * gate_ref[:, here].astype(f32)).astype(bf16)
        joined = jnp.concatenate([scaled, signal_ref[:, here]], 1)
        moved = dot(perm_ref[...], joined, ((1,), (1,)))
        pack[s] = moved.reshape(pieces, group, tokens).astype(bf16)

    pl.semaphore_wait(barrier, pieces)
    filter_copies = [
        peer_copy(pf.at[s], pfin.at[s], fsend.at[s], frecv.at[s], partner) for s in range(segments)
    ]
    for s in range(segments):
        filter_copies[s].start()
        start_exchange(pack.at[s], recv.at[s], send_in.at[s], recv_in.at[s])
    for n in range(5, 10):
        loads[n].wait()
    for s in range(segments):
        filter_copies[s].wait()
        for h in range(2):
            lanes = slice(h * HALF, (h + 1) * HALF)
            fs[s, h, pl.ds(other, part)] = pfin[s, :, lanes].astype(f32)

        def filter_step(n, carry, s=s):
            stages = []
            for c in (2 * n, 2 * n + 1):
                high, low = split(take(fs.at[s], c, rows, per_device))
                stages.append(
                    turn(dot(fwd_ref[...], jnp.concatenate([high, high, low], 0)), tw_ref)
                )
            at = pl.multiple_of(n * 2 * rows, 2 * rows)
            for p in range(2):
                fspec[s, p, pl.ds(at, 2 * rows)] = three(
                    jnp.concatenate([t[p] for t in stages], 0), in_ref, p
                )
            return carry

        lax.fori_loop(0, per_device // 2, filter_step, 0)

    short = fwd_ref[:, : 2 * rows]
    for s in range(segments):
        incoming = all_of(pack.at[s], recv.at[s], send_in.at[s], recv_in.at[s])
        incoming.wait_recv()
        for h in range(2):
            lanes = slice(h * HALF, (h + 1) * HALF)
            xs[h] = recv[s, :, :, lanes].astype(f32).reshape(rows * group, HALF)

        kernel_copy = peer_copy(kout.at[s], kbuf.at[s], ksend.at[s], krecv.at[s], partner)
        turned = []
        for c in range(per_device):
            for r in (c, c + per_device):
                x = take(xs, r, rows, group).astype(bf16)
                turned.append(turn(dot(short, jnp.concatenate([x, x], 0)), tw_ref))
        specs = [three(jnp.concatenate([t[p] for t in turned], 0), in_ref, p) for p in range(2)]

        def parts_of(p, c):
            g = specs[p][2 * c * rows : (2 * c + 1) * rows]
            x = specs[p][(2 * c + 1) * rows : (2 * c + 2) * rows]
            return g[:, :HALF], g[:, HALF:], x[:, :HALF], x[:, HALF:]

        def to_rows(products, targets):
            plus_minus = [three(jnp.concatenate(v, 0), inv_ref, p) for p, v in enumerate(products)]
            plus = plus_minus[0] + plus_minus[1]
            minus = plus_minus[0] - plus_minus[1]
            for n, target in enumerate(targets):
                here = slice(n * rows, (n + 1) * rows)
                high, low = split(unturn(plus[here], minus[here], tw_ref))
                put(*target, dot(inner_back_ref[...], jnp.concatenate([high, high, low], 0)))

        products = [[], []]
        for p in range(2):
            for c in range(per_device):
                gr, gi, sr, si = parts_of(p, c)
                products[p].append(
                    jnp.concatenate([gr * sr + gi * si, gi * sr - gr * si], 1)
                )
        to_rows(products, [(ks.at[s], c, rows, per_device) for c in range(per_device)])
        for h in range(2):
            lanes = slice(h * HALF, (h + 1) * HALF)
            kout[s, :, lanes] = ks[s, h, pl.ds(other, part)].astype(bf16)
        kernel_copy.start()

        products = [[], []]
        for p in range(2):
            for c in range(per_device):
                gr, gi, sr, si = parts_of(p, c)
                fr = fspec[s, p, c * rows : (c + 1) * rows, :HALF]
                fi = fspec[s, p, c * rows : (c + 1) * rows, HALF:]
                products[p] += [
                    jnp.concatenate([fr * gr + fi * gi, fr * gi - fi * gr], 1),
                    jnp.concatenate([fr * sr - fi * si, fr * si + fi * sr], 1),
                ]
        to_rows(
            products,
            [(ys, r, rows, group) for c in range(per_device) for r in (c, c + per_device)],
        )
        for h in range(2):
            lanes = slice(h * HALF, (h + 1) * HALF)
            back[s, :, :, lanes] = ys[h].reshape(pieces, group, HALF).astype(bf16)
        start_exchange(back.at[s], rec.at[s], send_out.at[s], recv_out.at[s])

    stores = []

    def store(n, s, at):
        copy = pltpu.make_async_copy(made[n].at[at], outs[n].at[at], store_sem.at[n, s])
        copy.start()
        stores.append(copy)

    for s in range(segments):
        peer_copy(kout.at[s], kbuf.at[s], ksend.at[s], krecv.at[s], partner).wait()
        for h in range(2):
            lanes = slice(h * HALF, (h + 1) * HALF)
            mine = ks[s, h, pl.ds(own, part)]
            ksum[h] = (mine + kbuf[s, :, lanes].astype(f32)) * factor
            for i in range(part // per_device):
                gf[s, :, i * U + h * HALF : i * U + (h + 1) * HALF] = ksum[
                    h, i * per_device : (i + 1) * per_device, :
                ]
        store(2, s, (s,))
        all_of(back.at[s], rec.at[s], send_out.at[s], recv_out.at[s]).wait_recv()
        here = slice(s * width, (s + 1) * width)
        arrived = rec[s].astype(f32).reshape(pieces * group, tokens).astype(bf16)
        both = dot(arrived, perm_ref[...], ((0,), (0,)))
        gs[:, here] = both[:, :width].astype(bf16)
        gg[:, here] = (grad_ref[:, here].astype(f32) * both[:, width:]).astype(bf16)
        at = (slice(None), pl.ds(s * width, width))
        store(0, s, at)
        store(1, s, at)
    for s in range(segments):
        all_of(pack.at[s], recv.at[s], send_in.at[s], recv_in.at[s]).wait_send()
        all_of(back.at[s], rec.at[s], send_out.at[s], recv_out.at[s]).wait_send()
    for copy in stores:
        copy.wait()


def finish_kernel(*refs):
    sources, outs, held = refs[:3], refs[3:6], refs[6:9]
    sems = refs[9]
    loads = [pltpu.make_async_copy(sources[n], held[n], sems.at[0, n]) for n in range(3)]
    stores = [pltpu.make_async_copy(held[n], outs[n], sems.at[1, n]) for n in range(3)]
    for copy in loads:
        copy.start()
    for n in range(3):
        loads[n].wait()
        stores[n].start()
    for copy in stores:
        copy.wait()


def hbm(count):
    return [pl.BlockSpec(memory_space=pltpu.HBM)] * count


def on_device(grad_out, gate, signal, filters):
    tokens, channels = grad_out.shape[1:]
    pieces = lax.axis_size("seq")
    halves = lax.axis_size("dp")
    segments, per_device, length = filters.shape
    group = 2 * per_device
    rows = length * halves // U
    part = length // U * per_device
    tables = [jnp.asarray(t) for t in make_tables(rows)]
    perm = jnp.asarray(make_permutation(pieces, per_device))
    gradient = grad_out[0]
    dma = pltpu.SemaphoreType.DMA
    blocks = (segments, pieces, group, tokens)
    operands = (gradient, gate[0], signal[0], filters, perm, *tables)
    factor = (halves * rows * U) ** (-0.5)
    results = (
        jax.ShapeDtypeStruct((tokens, channels), bf16),
        jax.ShapeDtypeStruct((tokens, channels), bf16),
        jax.ShapeDtypeStruct(filters.shape, f32),
    )
    made = pl.pallas_call(
        functools.partial(main_kernel, factor),
        out_shape=results,
        in_specs=hbm(10),
        out_specs=tuple(hbm(3)),
        scratch_shapes=[pltpu.VMEM(x.shape, x.dtype) for x in operands]
        + [
            pltpu.VMEM(blocks, bf16),
            pltpu.VMEM(blocks, bf16),
            pltpu.VMEM(blocks, bf16),
            pltpu.VMEM(blocks, bf16),
            pltpu.VMEM((segments, part, U), bf16),
            pltpu.VMEM((segments, part, U), bf16),
            pltpu.VMEM((segments, 2, rows * per_device, HALF), f32),
            pltpu.VMEM((segments, 2, rows * per_device, U), f32),
            pltpu.VMEM((2, rows * group, HALF), f32),
            pltpu.VMEM((2, rows * group, HALF), f32),
            pltpu.VMEM((segments, 2, rows * per_device, HALF), f32),
            pltpu.VMEM((2, part, HALF), f32),
            pltpu.VMEM((segments, part, U), bf16),
            pltpu.VMEM((segments, part, U), bf16),
            *[pltpu.VMEM(x.shape, x.dtype) for x in results],
            dma((segments,)),
            dma((segments,)),
            dma((segments,)),
            dma((segments,)),
            dma((segments,)),
            dma((segments,)),
            dma((segments,)),
            dma((segments,)),
            dma((len(operands),)),
            dma((3, segments)),
        ],
        compiler_params=pltpu.CompilerParams(
            collective_id=0, has_side_effects=True, vmem_limit_bytes=60 << 20
        ),
        name="main",
    )(*operands)
    grad_signal, grad_gate, grad_filter = pl.pallas_call(
        finish_kernel,
        out_shape=results,
        in_specs=hbm(3),
        out_specs=tuple(hbm(3)),
        scratch_shapes=[pltpu.VMEM(x.shape, x.dtype) for x in results] + [dma((2, 3))],
        name="finish",
    )(*made)
    return grad_signal[None], grad_gate[None], grad_filter


def solution(mesh):
    placed = (
        P("dp", "seq", None),
        P("dp", "seq", None),
        P("dp", "seq", None),
        P(None, "seq", "dp"),
    )
    return jax.shard_map(
        on_device,
        mesh=mesh,
        in_specs=placed,
        out_specs=(P("dp", "seq", None), P("dp", "seq", None), P(None, "seq", "dp")),
        check_vma=False,
    )
```

```python
import functools
import math

import jax
import jax.numpy as jnp
import numpy as np
from jax import lax
from jax.experimental import pallas as pl
from jax.experimental.pallas import tpu as pltpu
from jax.sharding import PartitionSpec as P

MESH = pl.DeviceIdType.MESH
bf16 = jnp.bfloat16
f32 = jnp.float32

U = 256
HALF = U // 2


def split_table(table):
    high = jnp.asarray(table, f32).astype(bf16)
    low = (jnp.asarray(table, f32) - high.astype(f32)).astype(bf16)
    return high, low


def np_bf16(table):
    import ml_dtypes

    return np.asarray(table, np.float32).astype(ml_dtypes.bfloat16)


def np_split(table):
    high = np_bf16(table)
    low = np_bf16(np.asarray(table, np.float64) - high.astype(np.float64))
    return high, low


@functools.lru_cache(None)
def make_tables(rows):
    points = 2 * rows * U
    k1 = np.arange(rows)[:, None]
    i = np.arange(rows)[None, :]
    angle = 2 * np.pi * (i * (2 * k1 + 1) % (4 * rows)) / (4 * rows)
    outer = np.concatenate([np.cos(angle), -np.sin(angle)], 0)
    high, low = np_split(outer)
    forward = np.concatenate([high, low, high], 1)
    back_high, back_low = np_split(outer.T * (2.0 / points))
    back = np.concatenate([back_high, back_low, back_high], 1)
    u = np.arange(U)[None, :]
    turn = 2 * np.pi * (u * (2 * k1 + 1)) / (2 * points)
    twiddle = np.stack([np.cos(turn), -np.sin(turn)]).astype(np.float32)
    u0 = np.arange(HALF)[:, None]
    m = np.arange(HALF)[None, :]
    inner = []
    for p in range(2):
        a = 2 * np.pi * (u0 * (2 * m + p) % U) / U
        c, s = np.cos(a), np.sin(a)
        inner.append(np.block([[c, -s], [s, c]]))
    inner = np.stack(inner)
    inner_tables = np.stack(np_split(inner), 1)
    inverse_tables = np.stack(np_split(np.swapaxes(inner, 1, 2)), 1)
    return forward, back, twiddle, inner_tables, inverse_tables


@functools.lru_cache(None)
def make_permutation(pieces, per_device):
    width = pieces * per_device
    row = np.arange(2 * width)
    j, rest = np.divmod(row, 2 * per_device)
    tensor, c = np.divmod(rest, per_device)
    table = np.zeros((2 * width, 2 * width), np.float32)
    table[row, tensor * width + j * per_device + c] = 1
    return np_bf16(table)


def dot(a, b, dims=((1,), (0,))):
    return lax.dot_general(a, b, (dims, ((), ())), preferred_element_type=f32)


def split(x):
    high = x.astype(bf16)
    return high, (x - high.astype(f32)).astype(bf16)


def peer_copy(src_ref, dst_ref, send_sem, recv_sem, peer):
    return pltpu.make_async_remote_copy(
        src_ref=src_ref,
        dst_ref=dst_ref,
        send_sem=send_sem,
        recv_sem=recv_sem,
        device_id=peer,
        device_id_type=MESH,
    )


def for_each_peer(visit):
    me = lax.axis_index("seq")
    far = (2, 3, 1, 0)

    def part(divisor, size):
        return lax.rem(lax.div(me, jnp.int32(divisor)), jnp.int32(size))

    core, x, y, z = part(1, 2), part(2, 4), part(8, 4), part(32, 2)
    low = [
        lax.rem(x + dx, jnp.int32(4)) * 2 + lax.rem(core + dc, jnp.int32(2))
        for dx in far
        for dc in (1, 0)
    ]
    z_other = (1 - z) * 32

    def row(base, targets):
        for target in targets:
            visit(base + target)

    def far_rows(n, carry):
        row(z_other + lax.rem(y + 2 + n, jnp.int32(4)) * 8, low)
        return carry

    def near_rows(n, carry):
        row(z * 32 + lax.rem(y + 1 + n, jnp.int32(4)) * 8, low)
        return carry

    lax.fori_loop(0, 4, far_rows, 0)
    lax.fori_loop(0, 3, near_rows, 0)
    row(z * 32 + y * 8, low[:-1])


def start_exchange(src_ref, dst_ref, send_sem, recv_sem):
    me = lax.axis_index("seq")

    def send(peer):
        peer_copy(
            src_ref.at[peer], dst_ref.at[me], send_sem, recv_sem, {"seq": peer}
        ).start()

    for_each_peer(send)
    dst_ref[me] = src_ref[me]


def all_of(src_ref, dst_ref, send_sem, recv_sem):
    others = pl.ds(0, src_ref.shape[0] - 1)
    return peer_copy(
        src_ref.at[others],
        dst_ref.at[others],
        send_sem,
        recv_sem,
        {"seq": lax.axis_index("seq")},
    )


def greet_all():
    barrier = pltpu.get_barrier_semaphore()

    def greet(peer):
        pl.semaphore_signal(barrier, inc=1, device_id={"seq": peer}, device_id_type=MESH)

    for_each_peer(greet)
    pl.semaphore_signal(
        barrier, inc=1, device_id={"dp": 1 - lax.axis_index("dp")}, device_id_type=MESH
    )
    return barrier


def take(ref, c, rows, stride):
    return jnp.concatenate([ref[h, pl.ds(c, rows, stride=stride), :] for h in range(2)], 1)


def put(ref, c, rows, stride, value):
    for h in range(2):
        ref[h, pl.ds(c, rows, stride=stride), :] = value[:, h * HALF : (h + 1) * HALF]


def turn(p, tw_ref):
    rows = p.shape[0] // 2
    pr, pi = p[:rows], p[rows:]
    tr, ti = tw_ref[0], tw_ref[1]
    qr = pr * tr - pi * ti
    qi = pr * ti + pi * tr
    a = jnp.concatenate([qr[:, :HALF], qi[:, :HALF]], 1)
    b = jnp.concatenate([qr[:, HALF:], qi[:, HALF:]], 1)
    return a + b, a - b


def unturn(plus, minus, tw_ref):
    tr, ti = tw_ref[0], tw_ref[1]
    zr = jnp.concatenate([plus[:, :HALF], minus[:, :HALF]], 1)
    zi = jnp.concatenate([plus[:, HALF:], minus[:, HALF:]], 1)
    return jnp.concatenate([zr * tr + zi * ti, zi * tr - zr * ti], 0)


def three(x, table_ref, p):
    high, low = split(x)
    return dot(high, table_ref[p, 0]) + dot(low, table_ref[p, 0]) + dot(high, table_ref[p, 1])


def main_kernel(factor, *refs):
    operands, refs = refs[:10], refs[10:]
    outs, refs = refs[:3], refs[3:]
    held, refs = refs[:10], refs[10:]
    grad_ref, gate_ref, signal_ref, filters_ref, perm_ref = held[:5]
    fwd_ref, inner_back_ref, tw_ref, in_ref, inv_ref = held[5:]
    pack, recv, back, rec, pf, pfin, fs, fspec, xs, ys, ks, ksum, kout, kbuf = refs[:14]
    made, refs = refs[14:17], refs[17:]
    gs, gg, gf = made
    send_in, recv_in, send_out, recv_out, fsend, frecv, ksend, krecv, load_sem, store_sem = refs
    segments, pieces, group, tokens = pack.shape
    per_device = group // 2
    rows = pieces * tokens // U
    part = pf.shape[1]
    dp = lax.axis_index("dp")
    partner = {"dp": 1 - dp}
    loads = [
        pltpu.make_async_copy(operands[n], held[n], load_sem.at[n]) for n in range(len(held))
    ]
    for n in (3, 0, 1, 2, 4, 5, 6, 7, 8, 9):
        loads[n].start()
    barrier = greet_all()

    loads[3].wait()
    own = dp * part
    other = (1 - dp) * part
    for s in range(segments):
        for i in range(part // per_device):
            for h in range(2):
                fs[s, h, pl.ds(own + i * per_device, per_device), :] = filters_ref[
                    s, :, i * U + h * HALF : i * U + (h + 1) * HALF
                ]
        for h in range(2):
            pf[s, :, h * HALF : (h + 1) * HALF] = fs[s, h, pl.ds(own, part)].astype(bf16)
    for n in (0, 1, 2, 4):
        loads[n].wait()
    width = pieces * per_device
    for s in range(segments):
        here = slice(s * width, (s + 1) * width)
        scaled = (grad_ref[:, here].astype(f32) * gate_ref[:, here].astype(f32)).astype(bf16)
        joined = jnp.concatenate([scaled, signal_ref[:, here]], 1)
        moved = dot(perm_ref[...], joined, ((1,), (1,)))
        pack[s] = moved.reshape(pieces, group, tokens).astype(bf16)

    pl.semaphore_wait(barrier, pieces)
    filter_copies = [
        peer_copy(pf.at[s], pfin.at[s], fsend.at[s], frecv.at[s], partner) for s in range(segments)
    ]
    filter_copies[0].start()
    start_exchange(pack.at[0], recv.at[0], send_in.at[0], recv_in.at[0])
    for s in range(1, segments):
        filter_copies[s].start()
    for n in range(5, 10):
        loads[n].wait()
    for s in range(segments):
        filter_copies[s].wait()
        if s + 1 < segments:
            start_exchange(pack.at[s + 1], recv.at[s + 1], send_in.at[s + 1], recv_in.at[s + 1])
        for h in range(2):
            lanes = slice(h * HALF, (h + 1) * HALF)
            fs[s, h, pl.ds(other, part)] = pfin[s, :, lanes].astype(f32)

        def filter_step(n, carry, s=s):
            stages = []
            for c in (2 * n, 2 * n + 1):
                high, low = split(take(fs.at[s], c, rows, per_device))
                stages.append(
                    turn(dot(fwd_ref[...], jnp.concatenate([high, high, low], 0)), tw_ref)
                )
            at = pl.multiple_of(n * 2 * rows, 2 * rows)
            for p in range(2):
                fspec[s, p, pl.ds(at, 2 * rows)] = three(
                    jnp.concatenate([t[p] for t in stages], 0), in_ref, p
                )
            return carry

        lax.fori_loop(0, per_device // 2, filter_step, 0)

    short = fwd_ref[:, : 2 * rows]
    for s in range(segments):
        incoming = all_of(pack.at[s], recv.at[s], send_in.at[s], recv_in.at[s])
        incoming.wait_recv()
        for h in range(2):
            lanes = slice(h * HALF, (h + 1) * HALF)
            xs[h] = recv[s, :, :, lanes].astype(f32).reshape(rows * group, HALF)

        kernel_copy = peer_copy(kout.at[s], kbuf.at[s], ksend.at[s], krecv.at[s], partner)
        turned = []
        for c in range(per_device):
            for r in (c, c + per_device):
                x = take(xs, r, rows, group).astype(bf16)
                turned.append(turn(dot(short, jnp.concatenate([x, x], 0)), tw_ref))
        specs = [three(jnp.concatenate([t[p] for t in turned], 0), in_ref, p) for p in range(2)]

        def parts_of(p, c):
            g = specs[p][2 * c * rows : (2 * c + 1) * rows]
            x = specs[p][(2 * c + 1) * rows : (2 * c + 2) * rows]
            return g[:, :HALF], g[:, HALF:], x[:, :HALF], x[:, HALF:]

        def to_rows(products, targets):
            plus_minus = [three(jnp.concatenate(v, 0), inv_ref, p) for p, v in enumerate(products)]
            plus = plus_minus[0] + plus_minus[1]
            minus = plus_minus[0] - plus_minus[1]
            for n, target in enumerate(targets):
                here = slice(n * rows, (n + 1) * rows)
                high, low = split(unturn(plus[here], minus[here], tw_ref))
                put(*target, dot(inner_back_ref[...], jnp.concatenate([high, high, low], 0)))

        products = [[], []]
        for p in range(2):
            for c in range(per_device):
                gr, gi, sr, si = parts_of(p, c)
                products[p].append(
                    jnp.concatenate([gr * sr + gi * si, gi * sr - gr * si], 1)
                )
        to_rows(products, [(ks.at[s], c, rows, per_device) for c in range(per_device)])
        for h in range(2):
            lanes = slice(h * HALF, (h + 1) * HALF)
            kout[s, :, lanes] = ks[s, h, pl.ds(other, part)].astype(bf16)
        kernel_copy.start()

        products = [[], []]
        for p in range(2):
            for c in range(per_device):
                gr, gi, sr, si = parts_of(p, c)
                fr = fspec[s, p, c * rows : (c + 1) * rows, :HALF]
                fi = fspec[s, p, c * rows : (c + 1) * rows, HALF:]
                products[p] += [
                    jnp.concatenate([fr * gr + fi * gi, fr * gi - fi * gr], 1),
                    jnp.concatenate([fr * sr - fi * si, fr * si + fi * sr], 1),
                ]
        to_rows(
            products,
            [(ys, r, rows, group) for c in range(per_device) for r in (c, c + per_device)],
        )
        for h in range(2):
            lanes = slice(h * HALF, (h + 1) * HALF)
            back[s, :, :, lanes] = ys[h].reshape(pieces, group, HALF).astype(bf16)
        start_exchange(back.at[s], rec.at[s], send_out.at[s], recv_out.at[s])

    stores = []

    def store(n, s, at):
        copy = pltpu.make_async_copy(made[n].at[at], outs[n].at[at], store_sem.at[n, s])
        copy.start()
        stores.append(copy)

    for s in range(segments):
        peer_copy(kout.at[s], kbuf.at[s], ksend.at[s], krecv.at[s], partner).wait()
        for h in range(2):
            lanes = slice(h * HALF, (h + 1) * HALF)
            mine = ks[s, h, pl.ds(own, part)]
            ksum[h] = (mine + kbuf[s, :, lanes].astype(f32)) * factor
            for i in range(part // per_device):
                gf[s, :, i * U + h * HALF : i * U + (h + 1) * HALF] = ksum[
                    h, i * per_device : (i + 1) * per_device, :
                ]
        store(2, s, (s,))
        all_of(back.at[s], rec.at[s], send_out.at[s], recv_out.at[s]).wait_recv()
        here = slice(s * width, (s + 1) * width)
        arrived = rec[s].astype(f32).reshape(pieces * group, tokens).astype(bf16)
        both = dot(arrived, perm_ref[...], ((0,), (0,)))
        gs[:, here] = both[:, :width].astype(bf16)
        gg[:, here] = (grad_ref[:, here].astype(f32) * both[:, width:]).astype(bf16)
        at = (slice(None), pl.ds(s * width, width))
        store(0, s, at)
        store(1, s, at)
    for s in range(segments):
        all_of(pack.at[s], recv.at[s], send_in.at[s], recv_in.at[s]).wait_send()
        all_of(back.at[s], rec.at[s], send_out.at[s], recv_out.at[s]).wait_send()
    for copy in stores:
        copy.wait()


def finish_kernel(*refs):
    sources, outs, held = refs[:3], refs[3:6], refs[6:9]
    sems = refs[9]
    loads = [pltpu.make_async_copy(sources[n], held[n], sems.at[0, n]) for n in range(3)]
    stores = [pltpu.make_async_copy(held[n], outs[n], sems.at[1, n]) for n in range(3)]
    for copy in loads:
        copy.start()
    for n in range(3):
        loads[n].wait()
        stores[n].start()
    for copy in stores:
        copy.wait()


def hbm(count):
    return [pl.BlockSpec(memory_space=pltpu.HBM)] * count


def on_device(grad_out, gate, signal, filters):
    tokens, channels = grad_out.shape[1:]
    pieces = lax.axis_size("seq")
    halves = lax.axis_size("dp")
    segments, per_device, length = filters.shape
    group = 2 * per_device
    rows = length * halves // U
    part = length // U * per_device
    tables = [jnp.asarray(t) for t in make_tables(rows)]
    perm = jnp.asarray(make_permutation(pieces, per_device))
    gradient = grad_out[0]
    dma = pltpu.SemaphoreType.DMA
    blocks = (segments, pieces, group, tokens)
    operands = (gradient, gate[0], signal[0], filters, perm, *tables)
    factor = (halves * rows * U) ** (-0.5)
    results = (
        jax.ShapeDtypeStruct((tokens, channels), bf16),
        jax.ShapeDtypeStruct((tokens, channels), bf16),
        jax.ShapeDtypeStruct(filters.shape, f32),
    )
    made = pl.pallas_call(
        functools.partial(main_kernel, factor),
        out_shape=results,
        in_specs=hbm(10),
        out_specs=tuple(hbm(3)),
        scratch_shapes=[pltpu.VMEM(x.shape, x.dtype) for x in operands]
        + [
            pltpu.VMEM(blocks, bf16),
            pltpu.VMEM(blocks, bf16),
            pltpu.VMEM(blocks, bf16),
            pltpu.VMEM(blocks, bf16),
            pltpu.VMEM((segments, part, U), bf16),
            pltpu.VMEM((segments, part, U), bf16),
            pltpu.VMEM((segments, 2, rows * per_device, HALF), f32),
            pltpu.VMEM((segments, 2, rows * per_device, U), f32),
            pltpu.VMEM((2, rows * group, HALF), f32),
            pltpu.VMEM((2, rows * group, HALF), f32),
            pltpu.VMEM((segments, 2, rows * per_device, HALF), f32),
            pltpu.VMEM((2, part, HALF), f32),
            pltpu.VMEM((segments, part, U), bf16),
            pltpu.VMEM((segments, part, U), bf16),
            *[pltpu.VMEM(x.shape, x.dtype) for x in results],
            dma((segments,)),
            dma((segments,)),
            dma((segments,)),
            dma((segments,)),
            dma((segments,)),
            dma((segments,)),
            dma((segments,)),
            dma((segments,)),
            dma((len(operands),)),
            dma((3, segments)),
        ],
        compiler_params=pltpu.CompilerParams(
            collective_id=0, has_side_effects=True, vmem_limit_bytes=60 << 20
        ),
        name="main",
    )(*operands)
    grad_signal, grad_gate, grad_filter = pl.pallas_call(
        finish_kernel,
        out_shape=results,
        in_specs=hbm(3),
        out_specs=tuple(hbm(3)),
        scratch_shapes=[pltpu.VMEM(x.shape, x.dtype) for x in results] + [dma((2, 3))],
        name="finish",
    )(*made)
    return grad_signal[None], grad_gate[None], grad_filter


def solution(mesh):
    placed = (
        P("dp", "seq", None),
        P("dp", "seq", None),
        P("dp", "seq", None),
        P(None, "seq", "dp"),
    )
    return jax.shard_map(
        on_device,
        mesh=mesh,
        in_specs=placed,
        out_specs=(P("dp", "seq", None), P("dp", "seq", None), P(None, "seq", "dp")),
        check_vma=False,
    )
```

```python
import functools
import math

import jax
import jax.numpy as jnp
import numpy as np
from jax import lax
from jax.experimental import pallas as pl
from jax.experimental.pallas import tpu as pltpu
from jax.sharding import PartitionSpec as P

MESH = pl.DeviceIdType.MESH
bf16 = jnp.bfloat16
f32 = jnp.float32

U = 256
HALF = U // 2


def split_table(table):
    high = jnp.asarray(table, f32).astype(bf16)
    low = (jnp.asarray(table, f32) - high.astype(f32)).astype(bf16)
    return high, low


def np_bf16(table):
    import ml_dtypes

    return np.asarray(table, np.float32).astype(ml_dtypes.bfloat16)


def np_split(table):
    high = np_bf16(table)
    low = np_bf16(np.asarray(table, np.float64) - high.astype(np.float64))
    return high, low


@functools.lru_cache(None)
def make_tables(rows):
    points = 2 * rows * U
    k1 = np.arange(rows)[:, None]
    i = np.arange(rows)[None, :]
    angle = 2 * np.pi * (i * (2 * k1 + 1) % (4 * rows)) / (4 * rows)
    outer = np.concatenate([np.cos(angle), -np.sin(angle)], 0)
    high, low = np_split(outer)
    forward = np.concatenate([high, low, high], 1)
    back_high, back_low = np_split(outer.T * (2.0 / points))
    back = np.concatenate([back_high, back_low, back_high], 1)
    u = np.arange(U)[None, :]
    turn = 2 * np.pi * (u * (2 * k1 + 1)) / (2 * points)
    twiddle = np.stack([np.cos(turn), -np.sin(turn)]).astype(np.float32)
    u0 = np.arange(HALF)[:, None]
    m = np.arange(HALF)[None, :]
    inner = []
    for p in range(2):
        a = 2 * np.pi * (u0 * (2 * m + p) % U) / U
        c, s = np.cos(a), np.sin(a)
        inner.append(np.block([[c, -s], [s, c]]))
    inner = np.stack(inner)
    inner_tables = np.stack(np_split(inner), 1)
    inverse_tables = np.stack(np_split(np.swapaxes(inner, 1, 2)), 1)
    return forward, back, twiddle, inner_tables, inverse_tables


@functools.lru_cache(None)
def make_permutation(pieces, per_device):
    width = pieces * per_device
    row = np.arange(2 * width)
    j, rest = np.divmod(row, 2 * per_device)
    tensor, c = np.divmod(rest, per_device)
    table = np.zeros((2 * width, 2 * width), np.float32)
    table[row, tensor * width + j * per_device + c] = 1
    return np_bf16(table)


def dot(a, b, dims=((1,), (0,))):
    return lax.dot_general(a, b, (dims, ((), ())), preferred_element_type=f32)


def split(x):
    high = x.astype(bf16)
    return high, (x - high.astype(f32)).astype(bf16)


def peer_copy(src_ref, dst_ref, send_sem, recv_sem, peer):
    return pltpu.make_async_remote_copy(
        src_ref=src_ref,
        dst_ref=dst_ref,
        send_sem=send_sem,
        recv_sem=recv_sem,
        device_id=peer,
        device_id_type=MESH,
    )


def for_each_peer(visit):
    me = lax.axis_index("seq")
    far = (2, 3, 1, 0)

    def part(divisor, size):
        return lax.rem(lax.div(me, jnp.int32(divisor)), jnp.int32(size))

    core, x, y, z = part(1, 2), part(2, 4), part(8, 4), part(32, 2)
    low = [
        lax.rem(x + dx, jnp.int32(4)) * 2 + lax.rem(core + dc, jnp.int32(2))
        for dx in far
        for dc in (1, 0)
    ]
    z_other = (1 - z) * 32

    def row(base, targets):
        for target in targets:
            visit(base + target)

    def far_rows(n, carry):
        row(z_other + lax.rem(y + 2 + n, jnp.int32(4)) * 8, low)
        return carry

    def near_rows(n, carry):
        row(z * 32 + lax.rem(y + 1 + n, jnp.int32(4)) * 8, low)
        return carry

    lax.fori_loop(0, 4, far_rows, 0)
    lax.fori_loop(0, 3, near_rows, 0)
    row(z * 32 + y * 8, low[:-1])


def start_exchange(src_ref, dst_ref, send_sem, recv_sem):
    me = lax.axis_index("seq")

    def send(peer):
        peer_copy(
            src_ref.at[peer], dst_ref.at[me], send_sem, recv_sem, {"seq": peer}
        ).start()

    for_each_peer(send)
    dst_ref[me] = src_ref[me]


def all_of(src_ref, dst_ref, send_sem, recv_sem):
    others = pl.ds(0, src_ref.shape[0] - 1)
    return peer_copy(
        src_ref.at[others],
        dst_ref.at[others],
        send_sem,
        recv_sem,
        {"seq": lax.axis_index("seq")},
    )


def greet_all():
    barrier = pltpu.get_barrier_semaphore()

    def greet(peer):
        pl.semaphore_signal(barrier, inc=1, device_id={"seq": peer}, device_id_type=MESH)

    for_each_peer(greet)
    pl.semaphore_signal(
        barrier, inc=1, device_id={"dp": 1 - lax.axis_index("dp")}, device_id_type=MESH
    )
    return barrier


def take(ref, c, rows, stride):
    return jnp.concatenate([ref[h, pl.ds(c, rows, stride=stride), :] for h in range(2)], 1)


def put(ref, c, rows, stride, value):
    for h in range(2):
        ref[h, pl.ds(c, rows, stride=stride), :] = value[:, h * HALF : (h + 1) * HALF]


def turn(p, tw_ref):
    rows = p.shape[0] // 2
    pr, pi = p[:rows], p[rows:]
    tr, ti = tw_ref[0], tw_ref[1]
    qr = pr * tr - pi * ti
    qi = pr * ti + pi * tr
    a = jnp.concatenate([qr[:, :HALF], qi[:, :HALF]], 1)
    b = jnp.concatenate([qr[:, HALF:], qi[:, HALF:]], 1)
    return a + b, a - b


def unturn(plus, minus, tw_ref):
    tr, ti = tw_ref[0], tw_ref[1]
    zr = jnp.concatenate([plus[:, :HALF], minus[:, :HALF]], 1)
    zi = jnp.concatenate([plus[:, HALF:], minus[:, HALF:]], 1)
    return jnp.concatenate([zr * tr + zi * ti, zi * tr - zr * ti], 0)


def three(x, table_ref, p):
    high, low = split(x)
    return dot(high, table_ref[p, 0]) + dot(low, table_ref[p, 0]) + dot(high, table_ref[p, 1])


def main_kernel(factor, *refs):
    operands, refs = refs[:10], refs[10:]
    outs, refs = refs[:3], refs[3:]
    held, refs = refs[:10], refs[10:]
    grad_ref, gate_ref, signal_ref, filters_ref, perm_ref = held[:5]
    fwd_ref, inner_back_ref, tw_ref, in_ref, inv_ref = held[5:]
    pack, recv, back, rec, pf, pfin, fs, fspec, xs, ys, ks, ksum, kout, kbuf = refs[:14]
    made, refs = refs[14:17], refs[17:]
    gs, gg, gf = made
    send_in, recv_in, send_out, recv_out, fsend, frecv, ksend, krecv, load_sem, store_sem = refs
    segments, pieces, group, tokens = pack.shape
    per_device = group // 2
    rows = pieces * tokens // U
    part = pf.shape[1]
    dp = lax.axis_index("dp")
    partner = {"dp": 1 - dp}
    loads = [
        pltpu.make_async_copy(operands[n], held[n], load_sem.at[n]) for n in range(len(held))
    ]
    for n in (3, 0, 1, 2, 4, 5, 6, 7, 8, 9):
        loads[n].start()
    barrier = greet_all()

    loads[3].wait()
    own = dp * part
    other = (1 - dp) * part
    for s in range(segments):
        for i in range(part // per_device):
            for h in range(2):
                fs[s, h, pl.ds(own + i * per_device, per_device), :] = filters_ref[
                    s, :, i * U + h * HALF : i * U + (h + 1) * HALF
                ]
        for h in range(2):
            pf[s, :, h * HALF : (h + 1) * HALF] = fs[s, h, pl.ds(own, part)].astype(bf16)
    for n in (0, 1, 2, 4):
        loads[n].wait()
    width = pieces * per_device
    for s in range(segments):
        here = slice(s * width, (s + 1) * width)
        scaled = (grad_ref[:, here].astype(f32) * gate_ref[:, here].astype(f32)).astype(bf16)
        joined = jnp.concatenate([scaled, signal_ref[:, here]], 1)
        moved = dot(perm_ref[...], joined, ((1,), (1,)))
        pack[s] = moved.reshape(pieces, group, tokens).astype(bf16)

    pl.semaphore_wait(barrier, pieces)
    filter_copies = [
        peer_copy(pf.at[s], pfin.at[s], fsend.at[s], frecv.at[s], partner) for s in range(segments)
    ]
    filter_copies[0].start()
    start_exchange(pack.at[0], recv.at[0], send_in.at[0], recv_in.at[0])
    for s in range(1, segments):
        filter_copies[s].start()
    for n in range(5, 10):
        loads[n].wait()
    short = fwd_ref[:, : 2 * rows]
    for s in range(segments):
        filter_copies[s].wait()
        if s + 1 < segments:
            start_exchange(pack.at[s + 1], recv.at[s + 1], send_in.at[s + 1], recv_in.at[s + 1])
        for h in range(2):
            lanes = slice(h * HALF, (h + 1) * HALF)
            fs[s, h, pl.ds(other, part)] = pfin[s, :, lanes].astype(f32)

        def filter_step(n, carry, s=s):
            stages = []
            for c in (2 * n, 2 * n + 1):
                high, low = split(take(fs.at[s], c, rows, per_device))
                stages.append(
                    turn(dot(fwd_ref[...], jnp.concatenate([high, high, low], 0)), tw_ref)
                )
            at = pl.multiple_of(n * 2 * rows, 2 * rows)
            for p in range(2):
                fspec[s, p, pl.ds(at, 2 * rows)] = three(
                    jnp.concatenate([t[p] for t in stages], 0), in_ref, p
                )
            return carry

        lax.fori_loop(0, per_device // 2, filter_step, 0)

        incoming = all_of(pack.at[s], recv.at[s], send_in.at[s], recv_in.at[s])
        incoming.wait_recv()
        for h in range(2):
            lanes = slice(h * HALF, (h + 1) * HALF)
            xs[h] = recv[s, :, :, lanes].astype(f32).reshape(rows * group, HALF)

        kernel_copy = peer_copy(kout.at[s], kbuf.at[s], ksend.at[s], krecv.at[s], partner)
        turned = []
        for c in range(per_device):
            for r in (c, c + per_device):
                x = take(xs, r, rows, group).astype(bf16)
                turned.append(turn(dot(short, jnp.concatenate([x, x], 0)), tw_ref))
        specs = [three(jnp.concatenate([t[p] for t in turned], 0), in_ref, p) for p in range(2)]

        def parts_of(p, c):
            g = specs[p][2 * c * rows : (2 * c + 1) * rows]
            x = specs[p][(2 * c + 1) * rows : (2 * c + 2) * rows]
            return g[:, :HALF], g[:, HALF:], x[:, :HALF], x[:, HALF:]

        def to_rows(products, targets):
            plus_minus = [three(jnp.concatenate(v, 0), inv_ref, p) for p, v in enumerate(products)]
            plus = plus_minus[0] + plus_minus[1]
            minus = plus_minus[0] - plus_minus[1]
            for n, target in enumerate(targets):
                here = slice(n * rows, (n + 1) * rows)
                high, low = split(unturn(plus[here], minus[here], tw_ref))
                put(*target, dot(inner_back_ref[...], jnp.concatenate([high, high, low], 0)))

        products = [[], []]
        for p in range(2):
            for c in range(per_device):
                gr, gi, sr, si = parts_of(p, c)
                products[p].append(
                    jnp.concatenate([gr * sr + gi * si, gi * sr - gr * si], 1)
                )
        to_rows(products, [(ks.at[s], c, rows, per_device) for c in range(per_device)])
        for h in range(2):
            lanes = slice(h * HALF, (h + 1) * HALF)
            kout[s, :, lanes] = ks[s, h, pl.ds(other, part)].astype(bf16)
        kernel_copy.start()

        products = [[], []]
        for p in range(2):
            for c in range(per_device):
                gr, gi, sr, si = parts_of(p, c)
                fr = fspec[s, p, c * rows : (c + 1) * rows, :HALF]
                fi = fspec[s, p, c * rows : (c + 1) * rows, HALF:]
                products[p] += [
                    jnp.concatenate([fr * gr + fi * gi, fr * gi - fi * gr], 1),
                    jnp.concatenate([fr * sr - fi * si, fr * si + fi * sr], 1),
                ]
        to_rows(
            products,
            [(ys, r, rows, group) for c in range(per_device) for r in (c, c + per_device)],
        )
        for h in range(2):
            lanes = slice(h * HALF, (h + 1) * HALF)
            back[s, :, :, lanes] = ys[h].reshape(pieces, group, HALF).astype(bf16)
        start_exchange(back.at[s], rec.at[s], send_out.at[s], recv_out.at[s])

    stores = []

    def store(n, s, at):
        copy = pltpu.make_async_copy(made[n].at[at], outs[n].at[at], store_sem.at[n, s])
        copy.start()
        stores.append(copy)

    for s in range(segments):
        peer_copy(kout.at[s], kbuf.at[s], ksend.at[s], krecv.at[s], partner).wait()
        for h in range(2):
            lanes = slice(h * HALF, (h + 1) * HALF)
            mine = ks[s, h, pl.ds(own, part)]
            ksum[h] = (mine + kbuf[s, :, lanes].astype(f32)) * factor
            for i in range(part // per_device):
                gf[s, :, i * U + h * HALF : i * U + (h + 1) * HALF] = ksum[
                    h, i * per_device : (i + 1) * per_device, :
                ]
        store(2, s, (s,))
        all_of(back.at[s], rec.at[s], send_out.at[s], recv_out.at[s]).wait_recv()
        here = slice(s * width, (s + 1) * width)
        arrived = rec[s].astype(f32).reshape(pieces * group, tokens).astype(bf16)
        both = dot(arrived, perm_ref[...], ((0,), (0,)))
        gs[:, here] = both[:, :width].astype(bf16)
        gg[:, here] = (grad_ref[:, here].astype(f32) * both[:, width:]).astype(bf16)
        at = (slice(None), pl.ds(s * width, width))
        store(0, s, at)
        store(1, s, at)
    for s in range(segments):
        all_of(pack.at[s], recv.at[s], send_in.at[s], recv_in.at[s]).wait_send()
        all_of(back.at[s], rec.at[s], send_out.at[s], recv_out.at[s]).wait_send()
    for copy in stores:
        copy.wait()


def finish_kernel(*refs):
    sources, outs, held = refs[:3], refs[3:6], refs[6:9]
    sems = refs[9]
    loads = [pltpu.make_async_copy(sources[n], held[n], sems.at[0, n]) for n in range(3)]
    stores = [pltpu.make_async_copy(held[n], outs[n], sems.at[1, n]) for n in range(3)]
    for copy in loads:
        copy.start()
    for n in range(3):
        loads[n].wait()
        stores[n].start()
    for copy in stores:
        copy.wait()


def hbm(count):
    return [pl.BlockSpec(memory_space=pltpu.HBM)] * count


def on_device(grad_out, gate, signal, filters):
    tokens, channels = grad_out.shape[1:]
    pieces = lax.axis_size("seq")
    halves = lax.axis_size("dp")
    segments, per_device, length = filters.shape
    group = 2 * per_device
    rows = length * halves // U
    part = length // U * per_device
    tables = [jnp.asarray(t) for t in make_tables(rows)]
    perm = jnp.asarray(make_permutation(pieces, per_device))
    gradient = grad_out[0]
    dma = pltpu.SemaphoreType.DMA
    blocks = (segments, pieces, group, tokens)
    operands = (gradient, gate[0], signal[0], filters, perm, *tables)
    factor = (halves * rows * U) ** (-0.5)
    results = (
        jax.ShapeDtypeStruct((tokens, channels), bf16),
        jax.ShapeDtypeStruct((tokens, channels), bf16),
        jax.ShapeDtypeStruct(filters.shape, f32),
    )
    made = pl.pallas_call(
        functools.partial(main_kernel, factor),
        out_shape=results,
        in_specs=hbm(10),
        out_specs=tuple(hbm(3)),
        scratch_shapes=[pltpu.VMEM(x.shape, x.dtype) for x in operands]
        + [
            pltpu.VMEM(blocks, bf16),
            pltpu.VMEM(blocks, bf16),
            pltpu.VMEM(blocks, bf16),
            pltpu.VMEM(blocks, bf16),
            pltpu.VMEM((segments, part, U), bf16),
            pltpu.VMEM((segments, part, U), bf16),
            pltpu.VMEM((segments, 2, rows * per_device, HALF), f32),
            pltpu.VMEM((segments, 2, rows * per_device, U), f32),
            pltpu.VMEM((2, rows * group, HALF), f32),
            pltpu.VMEM((2, rows * group, HALF), f32),
            pltpu.VMEM((segments, 2, rows * per_device, HALF), f32),
            pltpu.VMEM((2, part, HALF), f32),
            pltpu.VMEM((segments, part, U), bf16),
            pltpu.VMEM((segments, part, U), bf16),
            *[pltpu.VMEM(x.shape, x.dtype) for x in results],
            dma((segments,)),
            dma((segments,)),
            dma((segments,)),
            dma((segments,)),
            dma((segments,)),
            dma((segments,)),
            dma((segments,)),
            dma((segments,)),
            dma((len(operands),)),
            dma((3, segments)),
        ],
        compiler_params=pltpu.CompilerParams(
            collective_id=0, has_side_effects=True, vmem_limit_bytes=60 << 20
        ),
        name="main",
    )(*operands)
    grad_signal, grad_gate, grad_filter = pl.pallas_call(
        finish_kernel,
        out_shape=results,
        in_specs=hbm(3),
        out_specs=tuple(hbm(3)),
        scratch_shapes=[pltpu.VMEM(x.shape, x.dtype) for x in results] + [dma((2, 3))],
        name="finish",
    )(*made)
    return grad_signal[None], grad_gate[None], grad_filter


def solution(mesh):
    placed = (
        P("dp", "seq", None),
        P("dp", "seq", None),
        P("dp", "seq", None),
        P(None, "seq", "dp"),
    )
    return jax.shard_map(
        on_device,
        mesh=mesh,
        in_specs=placed,
        out_specs=(P("dp", "seq", None), P("dp", "seq", None), P(None, "seq", "dp")),
        check_vma=False,
    )
```

```python
import functools
import math

import jax
import jax.numpy as jnp
import numpy as np
from jax import lax
from jax.experimental import pallas as pl
from jax.experimental.pallas import tpu as pltpu
from jax.sharding import PartitionSpec as P

MESH = pl.DeviceIdType.MESH
bf16 = jnp.bfloat16
f32 = jnp.float32

U = 256
HALF = U // 2


def split_table(table):
    high = jnp.asarray(table, f32).astype(bf16)
    low = (jnp.asarray(table, f32) - high.astype(f32)).astype(bf16)
    return high, low


def np_bf16(table):
    import ml_dtypes

    return np.asarray(table, np.float32).astype(ml_dtypes.bfloat16)


def np_split(table):
    high = np_bf16(table)
    low = np_bf16(np.asarray(table, np.float64) - high.astype(np.float64))
    return high, low


@functools.lru_cache(None)
def make_tables(rows):
    points = 2 * rows * U
    k1 = np.arange(rows)[:, None]
    i = np.arange(rows)[None, :]
    angle = 2 * np.pi * (i * (2 * k1 + 1) % (4 * rows)) / (4 * rows)
    outer = np.concatenate([np.cos(angle), -np.sin(angle)], 0)
    high, low = np_split(outer)
    forward = np.concatenate([high, low, high], 1)
    back_high, back_low = np_split(outer.T * (2.0 / points))
    back = np.concatenate([back_high, back_low, back_high], 1)
    u = np.arange(U)[None, :]
    turn = 2 * np.pi * (u * (2 * k1 + 1)) / (2 * points)
    twiddle = np.stack([np.cos(turn), -np.sin(turn)]).astype(np.float32)
    u0 = np.arange(HALF)[:, None]
    m = np.arange(HALF)[None, :]
    inner = []
    for p in range(2):
        a = 2 * np.pi * (u0 * (2 * m + p) % U) / U
        c, s = np.cos(a), np.sin(a)
        inner.append(np.block([[c, -s], [s, c]]))
    inner = np.stack(inner)
    inner_tables = np.stack(np_split(inner), 1)
    inverse_tables = np.stack(np_split(np.swapaxes(inner, 1, 2)), 1)
    return forward, back, twiddle, inner_tables, inverse_tables


@functools.lru_cache(None)
def make_permutation(pieces, per_device):
    width = pieces * per_device
    row = np.arange(2 * width)
    j, rest = np.divmod(row, 2 * per_device)
    tensor, c = np.divmod(rest, per_device)
    table = np.zeros((2 * width, 2 * width), np.float32)
    table[row, tensor * width + j * per_device + c] = 1
    return np_bf16(table)


def dot(a, b, dims=((1,), (0,))):
    return lax.dot_general(a, b, (dims, ((), ())), preferred_element_type=f32)


def split(x):
    high = x.astype(bf16)
    return high, (x - high.astype(f32)).astype(bf16)


def peer_copy(src_ref, dst_ref, send_sem, recv_sem, peer):
    return pltpu.make_async_remote_copy(
        src_ref=src_ref,
        dst_ref=dst_ref,
        send_sem=send_sem,
        recv_sem=recv_sem,
        device_id=peer,
        device_id_type=MESH,
    )


def for_each_peer(visit):
    me = lax.axis_index("seq")
    far = (2, 3, 1, 0)

    def part(divisor, size):
        return lax.rem(lax.div(me, jnp.int32(divisor)), jnp.int32(size))

    core, x, y, z = part(1, 2), part(2, 4), part(8, 4), part(32, 2)
    low = [
        lax.rem(x + dx, jnp.int32(4)) * 2 + lax.rem(core + dc, jnp.int32(2))
        for dx in far
        for dc in (1, 0)
    ]
    z_other = (1 - z) * 32

    def row(base, targets):
        for target in targets:
            visit(base + target)

    def far_rows(n, carry):
        row(z_other + lax.rem(y + 2 + n, jnp.int32(4)) * 8, low)
        return carry

    def near_rows(n, carry):
        row(z * 32 + lax.rem(y + 1 + n, jnp.int32(4)) * 8, low)
        return carry

    lax.fori_loop(0, 4, far_rows, 0)
    lax.fori_loop(0, 3, near_rows, 0)
    row(z * 32 + y * 8, low[:-1])


def start_exchange(src_ref, dst_ref, send_sem, recv_sem):
    me = lax.axis_index("seq")

    def send(peer):
        peer_copy(
            src_ref.at[peer], dst_ref.at[me], send_sem, recv_sem, {"seq": peer}
        ).start()

    for_each_peer(send)
    dst_ref[me] = src_ref[me]


def all_of(src_ref, dst_ref, send_sem, recv_sem):
    others = pl.ds(0, src_ref.shape[0] - 1)
    return peer_copy(
        src_ref.at[others],
        dst_ref.at[others],
        send_sem,
        recv_sem,
        {"seq": lax.axis_index("seq")},
    )


def greet_all():
    barrier = pltpu.get_barrier_semaphore()

    def greet(peer):
        pl.semaphore_signal(barrier, inc=1, device_id={"seq": peer}, device_id_type=MESH)

    for_each_peer(greet)
    pl.semaphore_signal(
        barrier, inc=1, device_id={"dp": 1 - lax.axis_index("dp")}, device_id_type=MESH
    )
    return barrier


def take(ref, c, rows, stride):
    return jnp.concatenate([ref[h, pl.ds(c, rows, stride=stride), :] for h in range(2)], 1)


def put(ref, c, rows, stride, value):
    for h in range(2):
        ref[h, pl.ds(c, rows, stride=stride), :] = value[:, h * HALF : (h + 1) * HALF]


def turn(p, tw_ref):
    rows = p.shape[0] // 2
    pr, pi = p[:rows], p[rows:]
    tr, ti = tw_ref[0], tw_ref[1]
    qr = pr * tr - pi * ti
    qi = pr * ti + pi * tr
    a = jnp.concatenate([qr[:, :HALF], qi[:, :HALF]], 1)
    b = jnp.concatenate([qr[:, HALF:], qi[:, HALF:]], 1)
    return a + b, a - b


def unturn(plus, minus, tw_ref):
    tr, ti = tw_ref[0], tw_ref[1]
    zr = jnp.concatenate([plus[:, :HALF], minus[:, :HALF]], 1)
    zi = jnp.concatenate([plus[:, HALF:], minus[:, HALF:]], 1)
    return jnp.concatenate([zr * tr + zi * ti, zi * tr - zr * ti], 0)


def three(x, table_ref, p):
    high, low = split(x)
    return dot(high, table_ref[p, 0]) + dot(low, table_ref[p, 0]) + dot(high, table_ref[p, 1])


def main_kernel(factor, *refs):
    operands, refs = refs[:10], refs[10:]
    outs, refs = refs[:3], refs[3:]
    held, refs = refs[:10], refs[10:]
    grad_ref, gate_ref, signal_ref, filters_ref, perm_ref = held[:5]
    fwd_ref, inner_back_ref, tw_ref, in_ref, inv_ref = held[5:]
    pack, recv, back, rec, pf, pfin, fs, fspec, xs, ys, ks, ksum, kout, kbuf = refs[:14]
    made, refs = refs[14:17], refs[17:]
    gs, gg, gf = made
    send_in, recv_in, send_out, recv_out, fsend, frecv, ksend, krecv, load_sem, store_sem = refs
    segments, pieces, group, tokens = pack.shape
    per_device = group // 2
    rows = pieces * tokens // U
    part = pf.shape[1]
    dp = lax.axis_index("dp")
    partner = {"dp": 1 - dp}
    loads = [
        pltpu.make_async_copy(operands[n], held[n], load_sem.at[n]) for n in range(len(held))
    ]
    for n in (3, 0, 1, 2, 4, 5, 6, 7, 8, 9):
        loads[n].start()
    barrier = greet_all()

    own = dp * part
    other = (1 - dp) * part
    width = pieces * per_device

    def prepare_filter(s):
        for i in range(part // per_device):
            for h in range(2):
                fs[s, h, pl.ds(own + i * per_device, per_device), :] = filters_ref[
                    s, :, i * U + h * HALF : i * U + (h + 1) * HALF
                ]
        for h in range(2):
            pf[s, :, h * HALF : (h + 1) * HALF] = fs[s, h, pl.ds(own, part)].astype(bf16)

    def prepare_blocks(s):
        here = slice(s * width, (s + 1) * width)
        scaled = (grad_ref[:, here].astype(f32) * gate_ref[:, here].astype(f32)).astype(bf16)
        joined = jnp.concatenate([scaled, signal_ref[:, here]], 1)
        moved = dot(perm_ref[...], joined, ((1,), (1,)))
        pack[s] = moved.reshape(pieces, group, tokens).astype(bf16)

    filter_copies = [
        peer_copy(pf.at[s], pfin.at[s], fsend.at[s], frecv.at[s], partner) for s in range(segments)
    ]
    loads[3].wait()
    for s in range(segments):
        prepare_filter(s)
    for n in (0, 1, 2, 4):
        loads[n].wait()
    prepare_blocks(0)
    pl.semaphore_wait(barrier, pieces)
    filter_copies[0].start()
    start_exchange(pack.at[0], recv.at[0], send_in.at[0], recv_in.at[0])
    for s in range(1, segments):
        filter_copies[s].start()
        prepare_blocks(s)
    for n in range(5, 10):
        loads[n].wait()
    short = fwd_ref[:, : 2 * rows]
    for s in range(segments):
        filter_copies[s].wait()
        if s + 1 < segments:
            start_exchange(pack.at[s + 1], recv.at[s + 1], send_in.at[s + 1], recv_in.at[s + 1])
        for h in range(2):
            lanes = slice(h * HALF, (h + 1) * HALF)
            fs[s, h, pl.ds(other, part)] = pfin[s, :, lanes].astype(f32)

        def filter_step(n, carry, s=s):
            stages = []
            for c in (2 * n, 2 * n + 1):
                high, low = split(take(fs.at[s], c, rows, per_device))
                stages.append(
                    turn(dot(fwd_ref[...], jnp.concatenate([high, high, low], 0)), tw_ref)
                )
            at = pl.multiple_of(n * 2 * rows, 2 * rows)
            for p in range(2):
                fspec[s, p, pl.ds(at, 2 * rows)] = three(
                    jnp.concatenate([t[p] for t in stages], 0), in_ref, p
                )
            return carry

        lax.fori_loop(0, per_device // 2, filter_step, 0)

        incoming = all_of(pack.at[s], recv.at[s], send_in.at[s], recv_in.at[s])
        incoming.wait_recv()
        for h in range(2):
            lanes = slice(h * HALF, (h + 1) * HALF)
            xs[h] = recv[s, :, :, lanes].astype(f32).reshape(rows * group, HALF)

        kernel_copy = peer_copy(kout.at[s], kbuf.at[s], ksend.at[s], krecv.at[s], partner)
        turned = []
        for c in range(per_device):
            for r in (c, c + per_device):
                x = take(xs, r, rows, group).astype(bf16)
                turned.append(turn(dot(short, jnp.concatenate([x, x], 0)), tw_ref))
        specs = [three(jnp.concatenate([t[p] for t in turned], 0), in_ref, p) for p in range(2)]

        def parts_of(p, c):
            g = specs[p][2 * c * rows : (2 * c + 1) * rows]
            x = specs[p][(2 * c + 1) * rows : (2 * c + 2) * rows]
            return g[:, :HALF], g[:, HALF:], x[:, :HALF], x[:, HALF:]

        def to_rows(products, targets):
            plus_minus = [three(jnp.concatenate(v, 0), inv_ref, p) for p, v in enumerate(products)]
            plus = plus_minus[0] + plus_minus[1]
            minus = plus_minus[0] - plus_minus[1]
            for n, target in enumerate(targets):
                here = slice(n * rows, (n + 1) * rows)
                high, low = split(unturn(plus[here], minus[here], tw_ref))
                put(*target, dot(inner_back_ref[...], jnp.concatenate([high, high, low], 0)))

        products = [[], []]
        for p in range(2):
            for c in range(per_device):
                gr, gi, sr, si = parts_of(p, c)
                products[p].append(
                    jnp.concatenate([gr * sr + gi * si, gi * sr - gr * si], 1)
                )
        to_rows(products, [(ks.at[s], c, rows, per_device) for c in range(per_device)])
        for h in range(2):
            lanes = slice(h * HALF, (h + 1) * HALF)
            kout[s, :, lanes] = ks[s, h, pl.ds(other, part)].astype(bf16)
        kernel_copy.start()

        products = [[], []]
        for p in range(2):
            for c in range(per_device):
                gr, gi, sr, si = parts_of(p, c)
                fr = fspec[s, p, c * rows : (c + 1) * rows, :HALF]
                fi = fspec[s, p, c * rows : (c + 1) * rows, HALF:]
                products[p] += [
                    jnp.concatenate([fr * gr + fi * gi, fr * gi - fi * gr], 1),
                    jnp.concatenate([fr * sr - fi * si, fr * si + fi * sr], 1),
                ]
        to_rows(
            products,
            [(ys, r, rows, group) for c in range(per_device) for r in (c, c + per_device)],
        )
        for h in range(2):
            lanes = slice(h * HALF, (h + 1) * HALF)
            back[s, :, :, lanes] = ys[h].reshape(pieces, group, HALF).astype(bf16)
        start_exchange(back.at[s], rec.at[s], send_out.at[s], recv_out.at[s])

    stores = []

    def store(n, s, at):
        copy = pltpu.make_async_copy(made[n].at[at], outs[n].at[at], store_sem.at[n, s])
        copy.start()
        stores.append(copy)

    for s in range(segments):
        peer_copy(kout.at[s], kbuf.at[s], ksend.at[s], krecv.at[s], partner).wait()
        for h in range(2):
            lanes = slice(h * HALF, (h + 1) * HALF)
            mine = ks[s, h, pl.ds(own, part)]
            ksum[h] = (mine + kbuf[s, :, lanes].astype(f32)) * factor
            for i in range(part // per_device):
                gf[s, :, i * U + h * HALF : i * U + (h + 1) * HALF] = ksum[
                    h, i * per_device : (i + 1) * per_device, :
                ]
        store(2, s, (s,))
        all_of(back.at[s], rec.at[s], send_out.at[s], recv_out.at[s]).wait_recv()
        here = slice(s * width, (s + 1) * width)
        arrived = rec[s].astype(f32).reshape(pieces * group, tokens).astype(bf16)
        both = dot(arrived, perm_ref[...], ((0,), (0,)))
        gs[:, here] = both[:, :width].astype(bf16)
        gg[:, here] = (grad_ref[:, here].astype(f32) * both[:, width:]).astype(bf16)
        at = (slice(None), pl.ds(s * width, width))
        store(0, s, at)
        store(1, s, at)
    for s in range(segments):
        all_of(pack.at[s], recv.at[s], send_in.at[s], recv_in.at[s]).wait_send()
        all_of(back.at[s], rec.at[s], send_out.at[s], recv_out.at[s]).wait_send()
    for copy in stores:
        copy.wait()


def finish_kernel(*refs):
    sources, outs, held = refs[:3], refs[3:6], refs[6:9]
    sems = refs[9]
    loads = [pltpu.make_async_copy(sources[n], held[n], sems.at[0, n]) for n in range(3)]
    stores = [pltpu.make_async_copy(held[n], outs[n], sems.at[1, n]) for n in range(3)]
    for copy in loads:
        copy.start()
    for n in range(3):
        loads[n].wait()
        stores[n].start()
    for copy in stores:
        copy.wait()


def hbm(count):
    return [pl.BlockSpec(memory_space=pltpu.HBM)] * count


def on_device(grad_out, gate, signal, filters):
    tokens, channels = grad_out.shape[1:]
    pieces = lax.axis_size("seq")
    halves = lax.axis_size("dp")
    segments, per_device, length = filters.shape
    group = 2 * per_device
    rows = length * halves // U
    part = length // U * per_device
    tables = [jnp.asarray(t) for t in make_tables(rows)]
    perm = jnp.asarray(make_permutation(pieces, per_device))
    gradient = grad_out[0]
    dma = pltpu.SemaphoreType.DMA
    blocks = (segments, pieces, group, tokens)
    operands = (gradient, gate[0], signal[0], filters, perm, *tables)
    factor = (halves * rows * U) ** (-0.5)
    results = (
        jax.ShapeDtypeStruct((tokens, channels), bf16),
        jax.ShapeDtypeStruct((tokens, channels), bf16),
        jax.ShapeDtypeStruct(filters.shape, f32),
    )
    made = pl.pallas_call(
        functools.partial(main_kernel, factor),
        out_shape=results,
        in_specs=hbm(10),
        out_specs=tuple(hbm(3)),
        scratch_shapes=[pltpu.VMEM(x.shape, x.dtype) for x in operands]
        + [
            pltpu.VMEM(blocks, bf16),
            pltpu.VMEM(blocks, bf16),
            pltpu.VMEM(blocks, bf16),
            pltpu.VMEM(blocks, bf16),
            pltpu.VMEM((segments, part, U), bf16),
            pltpu.VMEM((segments, part, U), bf16),
            pltpu.VMEM((segments, 2, rows * per_device, HALF), f32),
            pltpu.VMEM((segments, 2, rows * per_device, U), f32),
            pltpu.VMEM((2, rows * group, HALF), f32),
            pltpu.VMEM((2, rows * group, HALF), f32),
            pltpu.VMEM((segments, 2, rows * per_device, HALF), f32),
            pltpu.VMEM((2, part, HALF), f32),
            pltpu.VMEM((segments, part, U), bf16),
            pltpu.VMEM((segments, part, U), bf16),
            *[pltpu.VMEM(x.shape, x.dtype) for x in results],
            dma((segments,)),
            dma((segments,)),
            dma((segments,)),
            dma((segments,)),
            dma((segments,)),
            dma((segments,)),
            dma((segments,)),
            dma((segments,)),
            dma((len(operands),)),
            dma((3, segments)),
        ],
        compiler_params=pltpu.CompilerParams(
            collective_id=0, has_side_effects=True, vmem_limit_bytes=60 << 20
        ),
        name="main",
    )(*operands)
    grad_signal, grad_gate, grad_filter = pl.pallas_call(
        finish_kernel,
        out_shape=results,
        in_specs=hbm(3),
        out_specs=tuple(hbm(3)),
        scratch_shapes=[pltpu.VMEM(x.shape, x.dtype) for x in results] + [dma((2, 3))],
        name="finish",
    )(*made)
    return grad_signal[None], grad_gate[None], grad_filter


def solution(mesh):
    placed = (
        P("dp", "seq", None),
        P("dp", "seq", None),
        P("dp", "seq", None),
        P(None, "seq", "dp"),
    )
    return jax.shard_map(
        on_device,
        mesh=mesh,
        in_specs=placed,
        out_specs=(P("dp", "seq", None), P("dp", "seq", None), P(None, "seq", "dp")),
        check_vma=False,
    )
```
